128 devices in a mesh: row: 16 (over y, z), col: 8 (over x, core).
Axes of the slice: x: 4, y: 4, z: 4, core: 2. Of those that a mesh axis runs over, the one named last changes fastest.
Arguments:
- queries: bfloat16 [49152, 4096], P(('row', 'col')), may hold values from -6 to 6
- keys: bfloat16 [65536, 256], P(('row', 'col')), may hold values from -6 to 6
- values: bfloat16 [65536, 256], P(('row', 'col')), may hold values from -6 to 6
- output_gradient: bfloat16 [49152, 4096], P(('row', 'col')), may hold values from -6 to 6
- tile_block_table: int32 [384, 3], P(('row', 'col')), may hold values from 0 to 127, as said below
Outputs:
- dqueries: bfloat16 [49152, 4096], P(('row', 'col'))
- dkeys: bfloat16 [65536, 256], P(('row', 'col'))
- dvalues: bfloat16 [65536, 256], P(('row', 'col'))
The draws below stay inside these ranges and needn't reach their ends.
Inputs may be any that keep to these rules, and one draw needn't show every extreme that they name: `tile_block_table`: A tile's first id is the block that holds its own query rows; its 3 ids are distinct and none is larger than that block. Block b is held by the device of index b // 1 in the order row-major over (row, col). The tiles of one device name at most 1 distinct blocks held on devices of one col index, and at most 2 distinct blocks held on devices of one row index.
All inputs are finite; a program needn't handle non-finite values.
Results may differ from the reference program's by a relative error of at most 0.0064.
Values may be sent and summed in bfloat16 or wider, within the bound.
A program may use at most 192 MiB of HBM per device.

```python
import jax
import jax.numpy as jnp
from jax import lax

QUERY_HEADS = 32
KEY_VALUE_HEADS = 2
HEAD_WIDTH = 128
GROUP_WIDTH = 16
TILE_QUERY_ROWS = 128
BLOCK_KEY_ROWS = 512
PICKED_BLOCKS = 3
BLK_DEV = 1
DEVICE_TILES = 3
CAP_COL = 1
CAP_ROW = 2
BLOCK_COUNT = 128
CONTEXT_LENGTH = 65536
TILES = 384
QROWS = 49152
N_ROW = 16
N_COL = 8


def draw_queries(key, part):
    gaussian_portion = jax.random.normal(jax.random.fold_in(key, 21), (QROWS, QUERY_HEADS, HEAD_WIDTH), jnp.float32)
    drawn_blocks = jnp.clip(gaussian_portion, -4.0, 4.0)
    return drawn_blocks.reshape(QROWS, QUERY_HEADS * HEAD_WIDTH).astype(jnp.bfloat16)


def draw_keys(key, part):
    gaussian_portion = jax.random.normal(jax.random.fold_in(key, 31), (CONTEXT_LENGTH, KEY_VALUE_HEADS, HEAD_WIDTH), jnp.float32)
    drawn_blocks = jnp.clip(gaussian_portion, -4.0, 4.0)
    return drawn_blocks.reshape(CONTEXT_LENGTH, KEY_VALUE_HEADS * HEAD_WIDTH).astype(jnp.bfloat16)


def device_lists(device_key, device):
    catalog = jnp.arange(BLOCK_COUNT, dtype=jnp.int32)
    holder = catalog // BLK_DEV
    holder_row = holder // N_COL
    holder_col = holder % N_COL
    same_row = (holder_row[None, :] == holder_row[:, None]).astype(jnp.int32)
    same_col = (holder_col[None, :] == holder_col[:, None]).astype(jnp.int32)
    tile_ids = device * DEVICE_TILES + jnp.arange(DEVICE_TILES, dtype=jnp.int32)
    own_blocks = (BLOCK_COUNT // 4 + tile_ids * TILE_QUERY_ROWS // BLOCK_KEY_ROWS).astype(jnp.int32)
    claimed = (catalog[None, :] == own_blocks[:, None]).astype(jnp.int32)
    chosen = jnp.max(claimed, axis=0)
    picked_ids = [own_blocks]
    for round_index in range(PICKED_BLOCKS - 1):
        column_picks = []
        for tile_index in range(DEVICE_TILES):
            round_key = jax.random.fold_in(device_key, round_index * DEVICE_TILES + tile_index)
            jitter = jax.random.randint(round_key, (BLOCK_COUNT,), 0, 4096)
            own_block = own_blocks[tile_index]
            reward = 2048 * (catalog == 0) + 1536 * (catalog == own_block - 1) + 1024 * (catalog == own_block - 2) + 1024 * chosen
            row_load = jnp.dot(same_row, chosen)
            col_load = jnp.dot(same_col, chosen)
            usable = (catalog < own_block) & (claimed[tile_index] == 0) & ((chosen == 1) | (row_load < CAP_ROW) & (col_load < CAP_COL))
            rating = jnp.where(usable, (reward + jitter) * BLOCK_COUNT + catalog, -1)
            picked = jnp.argmax(rating).astype(jnp.int32)
            marked = (catalog == picked).astype(jnp.int32)
            claimed = claimed.at[tile_index].set(jnp.maximum(claimed[tile_index], marked))
            chosen = jnp.maximum(chosen, marked)
            column_picks.append(picked)
        picked_ids.append(jnp.stack(column_picks))
    return jnp.stack(picked_ids, axis=1)


def draw_tile_block_table(key, part):
    device_keys = jax.random.split(key, N_ROW * N_COL)
    every_list = jax.vmap(device_lists)(device_keys, jnp.arange(N_ROW * N_COL, dtype=jnp.int32))
    return every_list.reshape(TILES, PICKED_BLOCKS).astype(jnp.int32)


def level_of(key, extent, pieces, low, largest):
    def one(axis_at, parts):
        draws = jax.random.uniform(jax.random.fold_in(jax.random.fold_in(key, 6), axis_at), (parts,), jnp.float32, low / len(pieces), largest / len(pieces))
        return jnp.repeat(jnp.exp(draws), extent[axis_at] // parts).reshape((-1,) + (1,) * (len(extent) - axis_at - 1))

    level = one(*pieces[0])
    for cut in pieces[1:]:
        level = level * one(*cut)
    return level


def normal_values(rng, dims, spread, most, shards=(), kind=jnp.bfloat16):
    result = jax.random.normal(rng, dims, jnp.float32) * spread
    if len(shards) > 0:
        result = level_of(rng, dims, shards, -0.22, 0.18) * result
    return jnp.clip(result, min=-most, max=most).astype(kind)


def setup_inputs(seed: int = 0) -> dict:
    key_of = jax.random.split(jax.random.key(seed), 6)
    return {
        "queries": draw_queries(jax.random.fold_in(key_of[5], 71), 0),
        "keys": draw_keys(jax.random.fold_in(key_of[5], 71), 0),
        "values": normal_values(key_of[2], (CONTEXT_LENGTH, KEY_VALUE_HEADS * HEAD_WIDTH), 1.0, 6.0, ((0, 128),)),
        "output_gradient": normal_values(key_of[3], (QROWS, QUERY_HEADS * HEAD_WIDTH), 1.0, 6.0, ((0, 128),)),
        "tile_block_table": draw_tile_block_table(jax.random.fold_in(key_of[5], 71), 0),
    }


def pair_grads(tile_query_rows, gradient_rows, block_key_rows, block_value_rows, query_place, key_place):
    factor = HEAD_WIDTH ** -0.5
    forward = (((1,), (1,)), ((), ()))
    backward = (((0,), (0,)), ((), ()))
    scores = lax.dot_general(tile_query_rows, block_key_rows, forward, preferred_element_type=jnp.float32) * factor
    scores = jnp.where(key_place[None, :] <= query_place[:, None], scores, -jnp.inf)
    weights = jax.nn.softmax(scores, axis=-1)
    grad_weights = lax.dot_general(gradient_rows, block_value_rows, forward, preferred_element_type=jnp.float32)
    row_delta = jnp.sum(weights * grad_weights, axis=-1, keepdims=True)
    grad_scores = (weights * (grad_weights - row_delta) * factor).astype(jnp.bfloat16)
    query_gradient = jnp.dot(grad_scores, block_key_rows, preferred_element_type=jnp.float32)
    key_gradient = lax.dot_general(grad_scores, tile_query_rows, backward, preferred_element_type=jnp.float32)
    value_gradient = lax.dot_general(weights.astype(jnp.bfloat16), gradient_rows, backward, preferred_element_type=jnp.float32)
    return query_gradient, key_gradient, value_gradient


def reference(queries, keys, values, output_gradient, tile_block_table):
    devices = N_ROW * N_COL
    starting_position = CONTEXT_LENGTH - QROWS
    key_block_grid = keys.reshape(BLOCK_COUNT, BLOCK_KEY_ROWS, KEY_VALUE_HEADS, HEAD_WIDTH)
    value_block_grid = values.reshape(BLOCK_COUNT, BLOCK_KEY_ROWS, KEY_VALUE_HEADS, HEAD_WIDTH)
    row_offsets = jnp.arange(BLOCK_KEY_ROWS, dtype=jnp.int32)
    rows_per_head = jnp.arange(GROUP_WIDTH * TILE_QUERY_ROWS, dtype=jnp.int32) % TILE_QUERY_ROWS

    def tile_step(tile_index):
        block_numbers = tile_block_table[tile_index]
        query_block_tile = lax.dynamic_slice_in_dim(queries, tile_index * TILE_QUERY_ROWS, TILE_QUERY_ROWS, 0)
        tile_gradient = lax.dynamic_slice_in_dim(output_gradient, tile_index * TILE_QUERY_ROWS, TILE_QUERY_ROWS, 0)
        tile_query_rows = query_block_tile.reshape(TILE_QUERY_ROWS, KEY_VALUE_HEADS, GROUP_WIDTH, HEAD_WIDTH).transpose(1, 2, 0, 3).reshape(KEY_VALUE_HEADS, GROUP_WIDTH * TILE_QUERY_ROWS, HEAD_WIDTH)
        gradient_rows = tile_gradient.reshape(TILE_QUERY_ROWS, KEY_VALUE_HEADS, GROUP_WIDTH, HEAD_WIDTH).transpose(1, 2, 0, 3).reshape(KEY_VALUE_HEADS, GROUP_WIDTH * TILE_QUERY_ROWS, HEAD_WIDTH)
        block_key_rows = key_block_grid[block_numbers].transpose(2, 0, 1, 3).reshape(KEY_VALUE_HEADS, PICKED_BLOCKS * BLOCK_KEY_ROWS, HEAD_WIDTH)
        block_value_rows = value_block_grid[block_numbers].transpose(2, 0, 1, 3).reshape(KEY_VALUE_HEADS, PICKED_BLOCKS * BLOCK_KEY_ROWS, HEAD_WIDTH)
        query_place = starting_position + tile_index * TILE_QUERY_ROWS + rows_per_head
        key_place = (block_numbers[:, None] * BLOCK_KEY_ROWS + row_offsets[None, :]).reshape(PICKED_BLOCKS * BLOCK_KEY_ROWS)
        query_gradient, key_gradient, value_gradient = jax.vmap(pair_grads, in_axes=(0, 0, 0, 0, None, None))(
            tile_query_rows, gradient_rows, block_key_rows, block_value_rows, query_place, key_place)
        query_gradient = query_gradient.reshape(KEY_VALUE_HEADS, GROUP_WIDTH, TILE_QUERY_ROWS, HEAD_WIDTH).transpose(2, 0, 1, 3).reshape(TILE_QUERY_ROWS, QUERY_HEADS * HEAD_WIDTH).astype(jnp.bfloat16)
        key_value_terms = jnp.stack((key_gradient, value_gradient), axis=0).reshape(2, KEY_VALUE_HEADS, PICKED_BLOCKS, BLOCK_KEY_ROWS, HEAD_WIDTH)
        key_value_terms = key_value_terms.transpose(2, 3, 0, 1, 4).reshape(PICKED_BLOCKS, BLOCK_KEY_ROWS * 2 * KEY_VALUE_HEADS * HEAD_WIDTH)
        return query_gradient, key_value_terms

    def per_device_body(running_totals, device):
        tile_range = device * DEVICE_TILES + jnp.arange(DEVICE_TILES, dtype=jnp.int32)
        query_gradient, key_value_terms = lax.map(tile_step, tile_range)
        block_numbers = lax.dynamic_slice_in_dim(tile_block_table, device * DEVICE_TILES, DEVICE_TILES, 0).reshape(DEVICE_TILES * PICKED_BLOCKS)
        paired_terms = key_value_terms.reshape(DEVICE_TILES * PICKED_BLOCKS, BLOCK_KEY_ROWS * 2 * KEY_VALUE_HEADS * HEAD_WIDTH)
        same_block = (block_numbers[:, None] == block_numbers[None, :]).astype(jnp.float32)
        first_seen = (jnp.sum(jnp.tril(same_block, -1), axis=1) == 0).astype(jnp.float32)
        merged = jnp.dot(same_block, paired_terms, precision=lax.Precision.HIGHEST, preferred_element_type=jnp.float32)
        rounded = lax.optimization_barrier(merged.astype(jnp.bfloat16)).astype(jnp.float32) * first_seen[:, None]
        running_totals = running_totals.at[block_numbers].add(rounded)
        return running_totals, query_gradient

    running_totals, query_gradients = lax.scan(per_device_body, jnp.zeros((BLOCK_COUNT, BLOCK_KEY_ROWS * 2 * KEY_VALUE_HEADS * HEAD_WIDTH), jnp.float32),
                                    jnp.arange(devices, dtype=jnp.int32))
    dqueries = query_gradients.reshape(QROWS, QUERY_HEADS * HEAD_WIDTH)
    overall_row_count = running_totals.reshape(CONTEXT_LENGTH, 2 * KEY_VALUE_HEADS * HEAD_WIDTH)
    return dqueries, overall_row_count[:, :KEY_VALUE_HEADS * HEAD_WIDTH].astype(jnp.bfloat16), overall_row_count[:, KEY_VALUE_HEADS * HEAD_WIDTH:].astype(jnp.bfloat16)
```

```python
import functools
import jax, jax.numpy as jnp
from jax import lax
from jax.experimental import pallas as pl
from jax.experimental.pallas import tpu as pltpu
HC=4
NT=(((1,),(1,)),((),()))
NN=(((1,),(0,)),((),()))
F32=jnp.float32; BF=jnp.bfloat16
def attn_kernel(hc, info, q_ref, do_ref, k_ref, v_ref, dq_ref, part_ref, acc):
    tile=pl.program_id(1)
    scale=128**-0.5
    c=scale*1.4426950408889634
    rows=hc*128
    @pl.when(tile==0)
    def _():
        acc[...]=jnp.zeros_like(acc)
    diag=info[18+tile]*128
    slots=[info[tile*3+j] for j in range(3)]
    def chunk(ci,_):
        off=pl.multiple_of(ci*rows,rows)
        q2=q_ref[:,pl.ds(off,rows)]; d2=do_ref[:,pl.ds(off,rows)]
        q=jnp.concatenate([q2[:,h*128:(h+1)*128] for h in range(hc)],axis=0)
        d=jnp.concatenate([d2[:,h*128:(h+1)*128] for h in range(hc)],axis=0)
        ks=[k_ref[slots[j]] for j in range(3)]
        vs=[v_ref[slots[j]] for j in range(3)]
        s=[lax.dot_general(q,ks[j],NT,preferred_element_type=F32) for j in range(3)]
        r=lax.broadcasted_iota(jnp.int32,(rows,512),0)&127
        col=lax.broadcasted_iota(jnp.int32,(rows,512),1)
        s[0]=jnp.where(col<=r+diag,s[0],-jnp.inf)
        m=jnp.max(jnp.maximum(jnp.maximum(s[0],s[1]),s[2]),axis=1,keepdims=True)*c
        p=[jnp.exp2(x*c-m) for x in s]
        l=jnp.sum(p[0]+p[1]+p[2],axis=1,keepdims=True)
        dp=[lax.dot_general(d,vs[j],NT,preferred_element_type=F32) for j in range(3)]
        t=jnp.sum(p[0]*dp[0]+p[1]*dp[1]+p[2]*dp[2],axis=1,keepdims=True)
        inv=1.0/l
        delta=t*inv
        ds=[(p[j]*(dp[j]-delta)).astype(BF) for j in range(3)]
        pb=[p[j].astype(BF) for j in range(3)]
        dq=sum(lax.dot_general(ds[j],ks[j],NN,preferred_element_type=F32) for j in range(3))
        dq=(dq*(inv*scale)).astype(BF)
        for h in range(hc):
            dq_ref[:,pl.ds(off+h*128,128)]=dq[h*128:(h+1)*128]
        qT=(q.astype(F32)*(inv*scale)).astype(BF).T
        dT=(d.astype(F32)*inv).astype(BF).T
        for j in range(3):
            acc[tile*3+j,0]+=lax.dot_general(qT,ds[j],NN,preferred_element_type=F32)
            acc[tile*3+j,1]+=lax.dot_general(dT,pb[j],NN,preferred_element_type=F32)
        return 0
    lax.fori_loop(0,16//hc,chunk,0)
    @pl.when(tile==2)
    def _():
        for sl in range(8):
            i0=info[24+sl]; i1=info[32+sl]; i2=info[40+sl]
            for kv in range(2):
                part_ref[sl,0,kv]=(acc[i0,kv]+acc[i1,kv]+acc[i2,kv]).astype(BF)
def make_info(table, my_device):
    slots=table%8
    tiles=my_device*3+jnp.arange(3,dtype=jnp.int32)
    hit=slots[:,None,:]==jnp.arange(8,dtype=jnp.int32)[None,:,None]
    ent=jnp.arange(9,dtype=jnp.int32).reshape(3,1,3)
    idx=jnp.min(jnp.where(hit,ent,9),axis=2)
    return jnp.concatenate([slots.reshape(9),jnp.zeros(9,jnp.int32),tiles%4,jnp.zeros(3,jnp.int32),idx.reshape(24)])
def attend(q,do,kv,info,hc=HC):
    return pl.pallas_call(
        functools.partial(attn_kernel,hc),
        grid_spec=pltpu.PrefetchScalarGridSpec(num_scalar_prefetch=1,grid=(2,3),
            in_specs=[pl.BlockSpec((128,2048),lambda g,t,_:(t,g)),
                      pl.BlockSpec((128,2048),lambda g,t,_:(t,g)),
                      pl.BlockSpec((None,8,512,128),lambda g,t,_:(2*g,0,0,0)),
                      pl.BlockSpec((None,8,512,128),lambda g,t,_:(2*g+1,0,0,0))],
            out_specs=[pl.BlockSpec((128,2048),lambda g,t,_:(t,g)),
                       pl.BlockSpec((8,1,2,128,512),lambda g,t,_:(0,g,0,0,0))],
            scratch_shapes=[pltpu.VMEM((10,2,128,512),F32)]),
        out_shape=[jax.ShapeDtypeStruct((384,4096),BF),jax.ShapeDtypeStruct((8,2,2,128,512),BF)],
        compiler_params=pltpu.CompilerParams(dimension_semantics=("arbitrary","arbitrary"),vmem_limit_bytes=60*2**20),
        cost_estimate=pl.CostEstimate(flops=24_000_000_000,bytes_accessed=20_000_000,transcendentals=19_000_000),
        name="attend",
    )(info,q,do,kv,kv)
BF=jnp.bfloat16; F32=jnp.float32
MESH=pl.DeviceIdType.MESH
OFFS=(0,-1,1,2)

class Place:
    def __init__(self):
        self.row=lax.axis_index("row"); self.col=lax.axis_index("col")
        self.y=self.row//4; self.z=self.row%4; self.x=self.col//2; self.core=self.col%2
    def rowid(self,first,da,db):
        dy,dz=(db,da) if first=="z" else (da,db)
        return ((self.y+dy+4)%4)*4+(self.z+dz+4)%4
    def colid(self,dx,core):
        return ((self.x+dx+4)%4)*2+core
    def barrier(self):
        sem=pltpu.get_barrier_semaphore()
        for d in (1,2,3,4,5,6,7):
            pl.semaphore_signal(sem,inc=1,device_id={"col":(self.col+d)%8},device_id_type=MESH)
        for dy,dz in ((1,0),(-1,0),(0,1),(0,-1)):
            pl.semaphore_signal(sem,inc=1,device_id={"row":((self.y+dy+4)%4)*4+(self.z+dz+4)%4},device_id_type=MESH)
        pl.semaphore_wait(sem,11)

class Wires:
    def __init__(self,ssem,rsem):
        self.ssem=ssem; self.rsem=rsem; self.pending=[]
    def send(self,src,dst,si,ri,where):
        d=pltpu.make_async_remote_copy(src_ref=src,dst_ref=dst,send_sem=self.ssem.at[si],recv_sem=self.rsem.at[ri],device_id=where,device_id_type=MESH)
        d.start(); self.pending.append(d)
    def got(self,dst,ri,where):
        pltpu.make_async_remote_copy(src_ref=dst,dst_ref=dst,send_sem=self.ssem.at[0],recv_sem=self.rsem.at[ri],device_id=where,device_id_type=MESH).wait_recv()
    def drain(self):
        for d in self.pending: d.wait_send()
        self.pending=[]

AG_SEMS=20
def gather_steps(me,w,own,buf,lo,n,first,base):
    full=pl.ds(lo,n); h0=pl.ds(lo,n//2); h1=pl.ds(lo+n//2,n//2)
    def at(da,db): return {"row":me.rowid(first,da,db)}
    def spread(o,src,dst):
        w.send(src,dst,base+4+o*4,base+4+o*4,at(0,1))
        w.send(src,dst,base+5+o*4,base+5+o*4,at(0,-1))
    def piece(da,db,rows): return buf.at[me.rowid(first,da,db),rows]
    def s0():
        w.send(own,piece(0,0,full),base,base,at(1,0))
        w.send(own,piece(0,0,full),base+1,base+1,at(-1,0))
        spread(0,own,piece(0,0,full))
    def s1():
        w.got(piece(-1,0,full),base,at(-1,0))
        w.send(piece(-1,0,h0),piece(-1,0,h0),base+2,base+2,at(1,0))
        spread(1,piece(-1,0,full),piece(-1,0,full))
        w.got(piece(1,0,full),base+1,at(1,0))
        w.send(piece(1,0,h1),piece(1,0,h1),base+3,base+3,at(-1,0))
        spread(2,piece(1,0,full),piece(1,0,full))
    def turn(o):
        da=OFFS[o]; b=base+4+o*4
        w.got(piece(da,-1,full),b,at(0,-1))
        w.send(piece(da,-1,h0),piece(da,-1,h0),b+2,b+2,at(0,1))
        w.got(piece(da,1,full),b+1,at(0,1))
        w.send(piece(da,1,h1),piece(da,1,h1),b+3,b+3,at(0,-1))
    def s2(): turn(0)
    def s3():
        w.got(piece(2,0,h0),base+2,at(-1,0))
        w.got(piece(2,0,h1),base+3,at(1,0))
        spread(3,piece(2,0,full),piece(2,0,full))
    def s4(): turn(1); turn(2)
    def s5(): turn(3)
    def s6():
        for o in range(4):
            b=base+4+o*4
            w.got(piece(OFFS[o],2,h0),b+2,at(0,-1))
            w.got(piece(OFFS[o],2,h1),b+3,at(0,1))
    return [s0,s1,s2,s3,s4,s5,s6]

A2A_SEMS=13
def exchange_steps(me,w,src,relay,land,n,base):
    h0=pl.ds(0,n//2); h1=pl.ds(n//2,n//2)
    x1=me.colid(1,me.core); xm=me.colid(-1,me.core)
    def e0():
        for k in range(2):
            far=src(me.colid(2,k))
            w.send(far.at[h0],relay.at[0,k],base+k,base+k,{"col":x1})
            w.send(far.at[h1],relay.at[1,k],base+2+k,base+2+k,{"col":xm})
        for k in range(2):
            w.send(src(me.colid(1,k)),land.at[me.col],base+4+k,base+4+me.core,{"col":me.colid(1,k)})
            w.send(src(me.colid(-1,k)),land.at[me.col],base+6+k,base+6+me.core,{"col":me.colid(-1,k)})
        w.send(src(me.colid(0,1-me.core)),land.at[me.col],base+8,base+8,{"col":me.colid(0,1-me.core)})
    def e1():
        for k in range(2):
            w.got(relay.at[0,k],base+k,{"col":xm})
            w.send(relay.at[0,k],land.at[xm,h0],base+9+k,base+9+me.core,{"col":me.colid(1,k)})
            w.got(relay.at[1,k],base+2+k,{"col":x1})
            w.send(relay.at[1,k],land.at[x1,h1],base+11+k,base+11+me.core,{"col":me.colid(-1,k)})
    def e2():
        for k in range(2):
            w.got(land.at[me.colid(-1,k)],base+4+k,{"col":me.colid(-1,k)})
            w.got(land.at[me.colid(1,k)],base+6+k,{"col":me.colid(1,k)})
        w.got(land.at[me.colid(0,1-me.core)],base+8,{"col":me.colid(0,1-me.core)})
        for k in range(2):
            w.got(land.at[me.colid(2,k),h0],base+9+k,{"col":me.colid(-1,k)})
            w.got(land.at[me.colid(2,k),h1],base+11+k,{"col":me.colid(1,k)})
    return [e0,e1,e2]

RS_SEMS=20
def reduce_steps(me,w,buf,t1,t2,c,c0,t3,t4,lo,n,first,base):
    full=pl.ds(lo,n); h0=pl.ds(lo,n//2); h1=pl.ds(lo+n//2,n//2); g0=pl.ds(0,n//2); g1=pl.ds(n//2,n//2)
    def at(da,db): return {"row":me.rowid(first,da,db)}
    def piece(da,db,rows): return buf.at[me.rowid(first,da,db),rows]
    order=(3,1,2,0)
    def add(ref,other):
        ref[...]=(ref[...].astype(F32)+other[...].astype(F32)).astype(BF)
    def r0():
        for o in order:
            b=base+o*4
            w.send(piece(2,OFFS[o],h0),t1.at[o,0],b,b,at(1,0))
            w.send(piece(2,OFFS[o],h1),t1.at[o,1],b+1,b+1,at(-1,0))
    def r1():
        for o in order:
            b=base+o*4
            w.got(t1.at[o,0],b,at(-1,0)); add(piece(1,OFFS[o],h0),t1.at[o,0])
            w.got(t1.at[o,1],b+1,at(1,0)); add(piece(-1,OFFS[o],h1),t1.at[o,1])
            w.send(piece(1,OFFS[o],full),t2.at[o,0],b+2,b+2,at(1,0))
            w.send(piece(-1,OFFS[o],full),t2.at[o,1],b+3,b+3,at(-1,0))
    def r2():
        for o in order:
            b=base+o*4
            w.got(t2.at[o,0],b+2,at(-1,0)); w.got(t2.at[o,1],b+3,at(1,0))
            total=piece(0,OFFS[o],full)[...].astype(F32)+t2[o,0].astype(F32)+t2[o,1].astype(F32)
            if o==0: c0[...]=total
            else: c[o]=total.astype(BF)
            if o==3:
                w.send(c.at[3,g0],t3.at[0],base+16,base+16,at(0,1))
                w.send(c.at[3,g1],t3.at[1],base+17,base+17,at(0,-1))
    def r3():
        w.got(t3.at[0],base+16,at(0,-1)); add(c.at[2,g0],t3.at[0])
        w.got(t3.at[1],base+17,at(0,1)); add(c.at[1,g1],t3.at[1])
        w.send(c.at[2],t4.at[0],base+18,base+18,at(0,1))
        w.send(c.at[1],t4.at[1],base+19,base+19,at(0,-1))
    def r4():
        w.got(t4.at[0],base+18,at(0,-1)); w.got(t4.at[1],base+19,at(0,1))
        c0[...]+=t4[0].astype(F32)+t4[1].astype(F32)
    return [r0,r1,r2,r3,r4]

def interleave(lists,lag):
    out=[]
    span=max(k*lag+len(l) for k,l in enumerate(lists))
    for t in range(span):
        for k,l in enumerate(lists):
            s=t-k*lag
            if 0<=s<len(l): out.append(l[s])
    return out

def fan_kernel(want_ref,k_ref,v_ref,kv_out,want_out,*scr):
    g=scr[0:4]; s=scr[4:8]; land=scr[8:12]; relay=scr[12]; wv,wsm,ssem,rsem,lsem=scr[13:]
    me=Place(); w=Wires(ssem,rsem)
    me.barrier()
    lb=4*(2*AG_SEMS+A2A_SEMS)
    for d in range(1,8):
        w.send(want_ref,wv.at[me.col],lb+d,lb+d,{"col":(me.col+d)%8})
    def src(q,lo,n):
        ref=(k_ref,v_ref)[q%2]
        return ref.at[pl.ds(lo,n),pl.ds((q//2)*128,128)]
    def lists():
        for d in range(1,8):
            w.got(wv.at[(me.col-d+8)%8],lb+d,{"col":(me.col-d+8)%8})
        a=pltpu.make_async_copy(wv,wsm,lsem.at[0]); a.start(); a.wait()
        b=pltpu.make_async_copy(want_ref,wsm.at[me.col],lsem.at[1]); b.start(); b.wait()
        want_out[...]=wv[...]
        want_out[me.col]=want_ref[...]
    todo=[]
    for q in range(4):
        base=q*(2*AG_SEMS+A2A_SEMS)
        A=gather_steps(me,w,src(q,0,256),g[q],0,256,"z",base)
        B=gather_steps(me,w,src(q,256,256),g[q],256,256,"y",base+AG_SEMS)
        both=[(lambda a=a,b=b:(a(),b())) for a,b in zip(A,B)]
        ex=exchange_steps(me,w,lambda c,q=q:s[q].at[c],relay.at[q],land[q],512,base+2*AG_SEMS)
        def pick(q=q):
            if q==0: lists()
            g[q][me.row]=src(q,0,512)[...]
            for c in range(8):
                rc=wsm[c,0,me.col]
                s[q][c]=g[q][rc]
            land[q][me.col]=s[q][me.col]
        def put(q=q):
            pltpu.make_async_copy(land[q],kv_out.at[q],lsem.at[2+q]).start()
        todo.append(both+[pick]+ex+[put])
    for f in interleave(todo,3): f()
    for q in range(4): pltpu.make_async_copy(land[q],kv_out.at[q],lsem.at[2+q]).wait()
    w.drain()

def fan_out(want,keys,values):
    n=4*(2*AG_SEMS+A2A_SEMS)+8
    return pl.pallas_call(fan_kernel,
        in_specs=[pl.BlockSpec(memory_space=pltpu.VMEM)]*3,
        out_specs=[pl.BlockSpec(memory_space=pl.ANY),pl.BlockSpec(memory_space=pltpu.VMEM)],
        out_shape=[jax.ShapeDtypeStruct((4,8,512,128),BF),jax.ShapeDtypeStruct((8,1,128),jnp.int32)],
        scratch_shapes=[pltpu.VMEM((16,512,128),BF)]*4+[pltpu.VMEM((8,512,128),BF)]*4+[pltpu.VMEM((8,512,128),BF)]*4+[
            pltpu.VMEM((4,2,2,256,128),BF),pltpu.VMEM((8,1,128),jnp.int32),pltpu.SMEM((8,1,128),jnp.int32),
            pltpu.SemaphoreType.DMA((n,)),pltpu.SemaphoreType.DMA((n,)),pltpu.SemaphoreType.DMA((6,))],
        compiler_params=pltpu.CompilerParams(collective_id=0,has_side_effects=True,vmem_limit_bytes=60*2**20),
        name="fan_out")(want,keys,values)

def fan_in_kernel(want_ref,part_ref,dk_ref,dv_ref,*scr):
    a=scr[0:4]; b=scr[4:8]; relay,t1,t2,c,c0,t3,t4,ssem,rsem=scr[8:]
    me=Place(); w=Wires(ssem,rsem)
    me.barrier()
    todo=[]
    for q in range(4):
        base=q*(2*RS_SEMS+A2A_SEMS); gg,kv=q//2,q%2
        ex=exchange_steps(me,w,lambda cc,gg=gg,kv=kv:part_ref.at[cc,gg,kv],relay.at[q],a[q],128,base+2*RS_SEMS)
        def merge(q=q,gg=gg,kv=kv):
            a[q][me.col]=part_ref[me.col,gg,kv]
            rows=[want_ref[cc,0,me.col] for cc in range(8)]
            def block(i,_):
                r=pl.ds(pl.multiple_of((i//2)*16,16),16); l=pl.ds(pl.multiple_of((i%2)*256,256),256)
                vals=[a[q][cc,r,l].astype(F32) for cc in range(8)]
                for R in range(16):
                    t=jnp.where(rows[0]==R,vals[0],0.0)
                    for cc in range(1,8): t=t+jnp.where(rows[cc]==R,vals[cc],0.0)
                    b[q][R,r,l]=t.astype(BF)
                return 0
            lax.fori_loop(0,16,block,0)
        A=reduce_steps(me,w,b[q],t1.at[q,0],t2.at[q,0],c.at[q,0],c0.at[q,0],t3.at[q,0],t4.at[q,0],0,64,"y",base)
        B=reduce_steps(me,w,b[q],t1.at[q,1],t2.at[q,1],c.at[q,1],c0.at[q,1],t3.at[q,1],t4.at[q,1],64,64,"z",base+RS_SEMS)
        both=[(lambda x=x,y=y:(x(),y())) for x,y in zip(A,B)]
        def fin(q=q,gg=gg,kv=kv):
            full=jnp.concatenate([c0[q,0],c0[q,1]],axis=0)
            (dk_ref,dv_ref)[kv][:,gg*128:(gg+1)*128]=full.T.astype(BF)
        todo.append(ex+[merge]+both+[fin])
    for f in interleave(todo,2): f()
    w.drain()

def fan_in(want_all,part):
    n=4*(2*RS_SEMS+A2A_SEMS)
    return pl.pallas_call(fan_in_kernel,
        in_specs=[pl.BlockSpec(memory_space=pltpu.SMEM),pl.BlockSpec(memory_space=pltpu.VMEM)],
        out_specs=[pl.BlockSpec(memory_space=pltpu.VMEM)]*2,
        out_shape=[jax.ShapeDtypeStruct((512,256),BF)]*2,
        scratch_shapes=[pltpu.VMEM((8,128,512),BF)]*4+[pltpu.VMEM((16,128,512),BF)]*4+[
            pltpu.VMEM((4,2,2,64,512),BF),pltpu.VMEM((4,2,4,2,32,512),BF),pltpu.VMEM((4,2,4,2,64,512),BF),
            pltpu.VMEM((4,2,4,64,512),BF),pltpu.VMEM((4,2,64,512),F32),pltpu.VMEM((4,2,2,32,512),BF),pltpu.VMEM((4,2,2,64,512),BF),
            pltpu.SemaphoreType.DMA((n,)),pltpu.SemaphoreType.DMA((n,))],
        compiler_params=pltpu.CompilerParams(collective_id=1,has_side_effects=True,vmem_limit_bytes=60*2**20),
        name="fan_in")(want_all,part)

def wants(table):
    hit=(table%8).reshape(9,1)==jnp.arange(8,dtype=jnp.int32)[None]
    rows=jnp.max(jnp.where(hit,(table//8).reshape(9,1),0),axis=0)
    return jnp.pad(rows,(0,120)).reshape(1,128)
def local(queries,keys,values,output_gradient,tile_block_table):
    me=lax.axis_index("row")*8+lax.axis_index("col")
    info=make_info(tile_block_table,me)
    kv,want_all=fan_out(wants(tile_block_table),keys,values)
    dq,part=attend(queries,output_gradient,kv,info)
    dk,dv=fan_in(want_all,part)
    return dq,dk,dv
def solution(mesh):
    from jax.sharding import PartitionSpec as P
    s=P(("row","col"),None)
    return jax.shard_map(local,mesh=mesh,in_specs=(s,)*5,out_specs=(s,)*3,check_vma=False)
```

```python
import functools
import jax, jax.numpy as jnp
from jax import lax
from jax.experimental import pallas as pl
from jax.experimental.pallas import tpu as pltpu
NT=(((1,),(1,)),((),()))
NN=(((1,),(0,)),((),()))
BF=jnp.bfloat16; F32=jnp.float32
MESH=pl.DeviceIdType.MESH
OFFS=(0,-1,1,2)

class Place:
    def __init__(self):
        self.row=lax.axis_index("row"); self.col=lax.axis_index("col")
        self.y=self.row//4; self.z=self.row%4; self.x=self.col//2; self.core=self.col%2
    def rowid(self,first,da,db):
        dy,dz=(db,da) if first=="z" else (da,db)
        return ((self.y+dy+4)%4)*4+(self.z+dz+4)%4
    def colid(self,dx,core):
        return ((self.x+dx+4)%4)*2+core
    def barrier(self):
        sem=pltpu.get_barrier_semaphore()
        for d in (1,2,3,4,5,6,7):
            pl.semaphore_signal(sem,inc=1,device_id={"col":(self.col+d)%8},device_id_type=MESH)
        for dy,dz in ((1,0),(-1,0),(0,1),(0,-1)):
            pl.semaphore_signal(sem,inc=1,device_id={"row":((self.y+dy+4)%4)*4+(self.z+dz+4)%4},device_id_type=MESH)
        pl.semaphore_wait(sem,11)

class Wires:
    def __init__(self,ssem,rsem):
        self.ssem=ssem; self.rsem=rsem; self.pending=[]
    def send(self,src,dst,si,ri,where):
        d=pltpu.make_async_remote_copy(src_ref=src,dst_ref=dst,send_sem=self.ssem.at[si],recv_sem=self.rsem.at[ri],device_id=where,device_id_type=MESH)
        d.start(); self.pending.append((src,si))
    def got(self,dst,ri,where):
        pltpu.make_async_remote_copy(src_ref=dst,dst_ref=dst,send_sem=self.ssem.at[0],recv_sem=self.rsem.at[ri],device_id=where,device_id_type=MESH).wait_recv()
    def drain(self):
        for src,si in self.pending:
            root=getattr(src,"ref",src); sh=src.shape
            ref=root.at[(0,)*(len(root.shape)-len(sh))+tuple(pl.ds(0,k) for k in sh)]
            near={"col":(lax.axis_index("col")+1)%8}
            pltpu.make_async_remote_copy(src_ref=ref,dst_ref=ref,send_sem=self.ssem.at[si],recv_sem=self.rsem.at[si],device_id=near,device_id_type=MESH).wait_send()
        self.pending=[]

AG_SEMS=20
def gather_steps(me,w,own,buf,lo,n,first,base):
    full=pl.ds(lo,n); h0=pl.ds(lo,n//2); h1=pl.ds(lo+n//2,n//2)
    def at(da,db): return {"row":me.rowid(first,da,db)}
    def spread(o,src,dst):
        w.send(src,dst,base+4+o*4,base+4+o*4,at(0,1))
        w.send(src,dst,base+5+o*4,base+5+o*4,at(0,-1))
    def piece(da,db,rows): return buf.at[me.rowid(first,da,db),rows]
    def s0():
        w.send(own,piece(0,0,full),base,base,at(1,0))
        w.send(own,piece(0,0,full),base+1,base+1,at(-1,0))
        spread(0,own,piece(0,0,full))
    def s1():
        w.got(piece(-1,0,full),base,at(-1,0))
        w.send(piece(-1,0,h0),piece(-1,0,h0),base+2,base+2,at(1,0))
        spread(1,piece(-1,0,full),piece(-1,0,full))
        w.got(piece(1,0,full),base+1,at(1,0))
        w.send(piece(1,0,h1),piece(1,0,h1),base+3,base+3,at(-1,0))
        spread(2,piece(1,0,full),piece(1,0,full))
    def turn(o):
        da=OFFS[o]; b=base+4+o*4
        w.got(piece(da,-1,full),b,at(0,-1))
        w.send(piece(da,-1,h0),piece(da,-1,h0),b+2,b+2,at(0,1))
        w.got(piece(da,1,full),b+1,at(0,1))
        w.send(piece(da,1,h1),piece(da,1,h1),b+3,b+3,at(0,-1))
    def s2(): turn(0)
    def s3():
        w.got(piece(2,0,h0),base+2,at(-1,0))
        w.got(piece(2,0,h1),base+3,at(1,0))
        spread(3,piece(2,0,full),piece(2,0,full))
    def s4(): turn(1); turn(2)
    def s5(): turn(3)
    def s6():
        for o in range(4):
            b=base+4+o*4
            w.got(piece(OFFS[o],2,h0),b+2,at(0,-1))
            w.got(piece(OFFS[o],2,h1),b+3,at(0,1))
    return [s0,s1,s2,s3,s4,s5,s6]

A2A_SEMS=13
def exchange_steps(me,w,src,relay,land,n,base):
    h0=pl.ds(0,n//2); h1=pl.ds(n//2,n//2)
    x1=me.colid(1,me.core); xm=me.colid(-1,me.core)
    def e0():
        for k in range(2):
            far=src(me.colid(2,k))
            w.send(far.at[h0],relay.at[0,k],base+k,base+k,{"col":x1})
            w.send(far.at[h1],relay.at[1,k],base+2+k,base+2+k,{"col":xm})
        for k in range(2):
            w.send(src(me.colid(1,k)),land.at[me.col],base+4+k,base+4+me.core,{"col":me.colid(1,k)})
            w.send(src(me.colid(-1,k)),land.at[me.col],base+6+k,base+6+me.core,{"col":me.colid(-1,k)})
        w.send(src(me.colid(0,1-me.core)),land.at[me.col],base+8,base+8,{"col":me.colid(0,1-me.core)})
    def e1():
        for k in range(2):
            w.got(relay.at[0,k],base+k,{"col":xm})
            w.send(relay.at[0,k],land.at[xm,h0],base+9+k,base+9+me.core,{"col":me.colid(1,k)})
            w.got(relay.at[1,k],base+2+k,{"col":x1})
            w.send(relay.at[1,k],land.at[x1,h1],base+11+k,base+11+me.core,{"col":me.colid(-1,k)})
    def e2():
        for k in range(2):
            w.got(land.at[me.colid(-1,k)],base+4+k,{"col":me.colid(-1,k)})
            w.got(land.at[me.colid(1,k)],base+6+k,{"col":me.colid(1,k)})
        w.got(land.at[me.colid(0,1-me.core)],base+8,{"col":me.colid(0,1-me.core)})
        for k in range(2):
            w.got(land.at[me.colid(2,k),h0],base+9+k,{"col":me.colid(-1,k)})
            w.got(land.at[me.colid(2,k),h1],base+11+k,{"col":me.colid(1,k)})
    return [e0,e1,e2]

RS_SEMS=20
def reduce_steps(me,w,buf,t1,t2,c,c0,t3,t4,lo,n,first,base):
    full=pl.ds(lo,n); h0=pl.ds(lo,n//2); h1=pl.ds(lo+n//2,n//2); g0=pl.ds(0,n//2); g1=pl.ds(n//2,n//2)
    def at(da,db): return {"row":me.rowid(first,da,db)}
    def piece(da,db,rows): return buf.at[me.rowid(first,da,db),rows]
    order=(3,1,2,0)
    def add(ref,other):
        ref[...]=(ref[...].astype(F32)+other[...].astype(F32)).astype(BF)
    def r0():
        for o in order:
            b=base+o*4
            w.send(piece(2,OFFS[o],h0),t1.at[o,0],b,b,at(1,0))
            w.send(piece(2,OFFS[o],h1),t1.at[o,1],b+1,b+1,at(-1,0))
    def r1():
        for o in order:
            b=base+o*4
            w.got(t1.at[o,0],b,at(-1,0)); add(piece(1,OFFS[o],h0),t1.at[o,0])
            w.got(t1.at[o,1],b+1,at(1,0)); add(piece(-1,OFFS[o],h1),t1.at[o,1])
            w.send(piece(1,OFFS[o],full),t2.at[o,0],b+2,b+2,at(1,0))
            w.send(piece(-1,OFFS[o],full),t2.at[o,1],b+3,b+3,at(-1,0))
    def r2():
        for o in order:
            b=base+o*4
            w.got(t2.at[o,0],b+2,at(-1,0)); w.got(t2.at[o,1],b+3,at(1,0))
            total=piece(0,OFFS[o],full)[...].astype(F32)+t2[o,0].astype(F32)+t2[o,1].astype(F32)
            if o==0: c0[...]=total
            else: c[o]=total.astype(BF)
            if o==3:
                w.send(c.at[3,g0],t3.at[0],base+16,base+16,at(0,1))
                w.send(c.at[3,g1],t3.at[1],base+17,base+17,at(0,-1))
    def r3():
        w.got(t3.at[0],base+16,at(0,-1)); add(c.at[2,g0],t3.at[0])
        w.got(t3.at[1],base+17,at(0,1)); add(c.at[1,g1],t3.at[1])
        w.send(c.at[2],t4.at[0],base+18,base+18,at(0,1))
        w.send(c.at[1],t4.at[1],base+19,base+19,at(0,-1))
    def r4():
        w.got(t4.at[0],base+18,at(0,-1)); w.got(t4.at[1],base+19,at(0,1))
        c0[...]+=t4[0].astype(F32)+t4[1].astype(F32)
    return [r0,r1,r2,r3,r4]

def interleave(lists,lag):
    out=[]
    span=max(k*lag+len(l) for k,l in enumerate(lists))
    for t in range(span):
        for k,l in enumerate(lists):
            s=t-k*lag
            if 0<=s<len(l): out.append(l[s])
    return out

def make_info(table, my_device):
    slots=table%8
    tiles=my_device*3+jnp.arange(3,dtype=jnp.int32)
    hit=slots[:,None,:]==jnp.arange(8,dtype=jnp.int32)[None,:,None]
    ent=jnp.arange(9,dtype=jnp.int32).reshape(3,1,3)
    idx=jnp.min(jnp.where(hit,ent,9),axis=2)
    return jnp.concatenate([slots.reshape(9),jnp.zeros(9,jnp.int32),tiles%4,jnp.zeros(3,jnp.int32),idx.reshape(24)])
HC=2
NCH=16//HC
ITERS=3*NCH
LB=4*(2*AG_SEMS+A2A_SEMS)
IB=LB+8
NSEM=IB+4*(2*RS_SEMS+A2A_SEMS)

def attend_unit(g,it,hc,info,qb,db,kb,vb,acc):
    scale=128**-0.5
    c=scale*1.4426950408889634
    rows=hc*128
    tile=it//NCH
    off=pl.multiple_of(g*2048+(it%NCH)*rows,rows)
    rsl=pl.ds(pl.multiple_of(tile*128,128),128)
    diag=info[18+tile]*128
    slots=[info[tile*3+j] for j in range(3)]
    q2=qb[rsl,pl.ds(off,rows)]; d2=db[rsl,pl.ds(off,rows)]
    q=jnp.concatenate([q2[:,h*128:(h+1)*128] for h in range(hc)],axis=0)
    d=jnp.concatenate([d2[:,h*128:(h+1)*128] for h in range(hc)],axis=0)
    ks=[kb[slots[j]] for j in range(3)]
    vs=[vb[slots[j]] for j in range(3)]
    s=[lax.dot_general(q,ks[j],NT,preferred_element_type=F32) for j in range(3)]
    r=lax.broadcasted_iota(jnp.int32,(rows,512),0)&127
    col=lax.broadcasted_iota(jnp.int32,(rows,512),1)
    s[0]=jnp.where(col<=r+diag,s[0],-jnp.inf)
    m=jnp.max(jnp.maximum(jnp.maximum(s[0],s[1]),s[2]),axis=1,keepdims=True)*c
    p=[jnp.exp2(x*c-m) for x in s]
    l=jnp.sum(p[0]+p[1]+p[2],axis=1,keepdims=True)
    dp=[lax.dot_general(d,vs[j],NT,preferred_element_type=F32) for j in range(3)]
    t=jnp.sum(p[0]*dp[0]+p[1]*dp[1]+p[2]*dp[2],axis=1,keepdims=True)
    inv=1.0/l
    delta=t*inv
    p=[p[j]*inv for j in range(3)]
    ds=[(p[j]*(dp[j]-delta)*scale).astype(BF) for j in range(3)]
    pb=[p[j].astype(BF) for j in range(3)]
    dq=sum(lax.dot_general(ds[j],ks[j],NN,preferred_element_type=F32) for j in range(3)).astype(BF)
    for h in range(hc):
        qb[rsl,pl.ds(off+h*128,128)]=dq[h*128:(h+1)*128]
    qT=q.T
    dT=d.T
    for j in range(3):
        acc[tile*3+j,0]+=lax.dot_general(qT,ds[j],NN,preferred_element_type=F32)
        acc[tile*3+j,1]+=lax.dot_general(dT,pb[j],NN,preferred_element_type=F32)

def mega_kernel(info,want_ref,k_ref,v_ref,q_hbm,do_hbm,dq_hbm,dk_ref,dv_ref,*scr):
    scr=list(scr)
    take=lambda n:[scr.pop(0) for _ in range(n)]
    gat=take(4); pickd=take(2); land=take(4); relay1,wv,wsm=take(3)
    qb,db,acc=take(3); part=take(2); back=take(4); sums=take(2)
    relay2,t1,t2,c,c0,t3,t4=take(7); ssem,rsem,lsem=take(3)
    me=Place(); w=Wires(ssem,rsem)
    qc=pltpu.make_async_copy(q_hbm,qb,lsem.at[2]); qc.start()
    dc=pltpu.make_async_copy(do_hbm,db,lsem.at[3]); dc.start()
    me.barrier()
    for d in range(1,8):
        w.send(want_ref,wv.at[me.col],LB+d,LB+d,{"col":(me.col+d)%8})
    def src(q,lo,n):
        return (k_ref,v_ref)[q%2].at[pl.ds(lo,n),pl.ds((q//2)*128,128)]
    def lists():
        for d in range(1,8):
            w.got(wv.at[(me.col-d+8)%8],LB+d,{"col":(me.col-d+8)%8})
        a=pltpu.make_async_copy(wv,wsm,lsem.at[0]); a.start(); a.wait()
        b=pltpu.make_async_copy(want_ref,wsm.at[me.col],lsem.at[1]); b.start(); b.wait()
    exw=[Wires(ssem,rsem) for _ in range(4)]
    out=[]
    for q in range(4):
        base=q*(2*AG_SEMS+A2A_SEMS)
        A=gather_steps(me,w,src(q,0,256),gat[q],0,256,"z",base)
        B=gather_steps(me,w,src(q,256,256),gat[q],256,256,"y",base+AG_SEMS)
        both=[(lambda a=a,b=b:(a(),b())) for a,b in zip(A,B)]
        ex=exchange_steps(me,exw[q],lambda cc,q=q:pickd[q%2].at[cc],relay1.at[q],land[q],512,base+2*AG_SEMS)
        def pick(q=q):
            if q==0: lists()
            if q>=2: exw[q-2].drain()
            gat[q][me.row]=src(q,0,512)[...]
            for cc in range(8):
                pickd[q%2][cc]=gat[q][wsm[cc,0,me.col]]
            land[q][me.col]=pickd[q%2][me.col]
        out.append(both+[pick]+ex)
    n=len(out[0])
    redw=[Wires(ssem,rsem) for _ in range(4)]
    ret=[]
    for q in range(4):
        base=IB+q*(2*RS_SEMS+A2A_SEMS); gg,kv=q//2,q%2
        ex=exchange_steps(me,w,lambda cc,gg=gg,kv=kv:part[gg].at[cc,kv],relay2.at[q],back[q],128,base+2*RS_SEMS)
        def merge(q=q,gg=gg,kv=kv):
            if q>=2: redw[q-2].drain()
            a=back[q]; b=sums[q%2]
            a[me.col]=part[gg][me.col,kv]
            rows=[wsm[cc,0,me.col] for cc in range(8)]
            def block(i,_):
                r=pl.ds(pl.multiple_of((i//2)*16,16),16); ln=pl.ds(pl.multiple_of((i%2)*256,256),256)
                vals=[a[cc,r,ln].astype(F32) for cc in range(8)]
                for R in range(16):
                    t=jnp.where(rows[0]==R,vals[0],0.0)
                    for cc in range(1,8): t=t+jnp.where(rows[cc]==R,vals[cc],0.0)
                    b[R,r,ln]=t.astype(BF)
                return 0
            lax.fori_loop(0,16,block,0)
        A=reduce_steps(me,redw[q],sums[q%2],t1.at[q,0],t2.at[q,0],c.at[q,0],c0.at[0],t3.at[q,0],t4.at[q,0],0,64,"y",base)
        B=reduce_steps(me,redw[q],sums[q%2],t1.at[q,1],t2.at[q,1],c.at[q,1],c0.at[1],t3.at[q,1],t4.at[q,1],64,64,"z",base+RS_SEMS)
        both=[(lambda x=x,y=y:(x(),y())) for x,y in zip(A,B)]
        def fin(q=q,gg=gg,kv=kv):
            (dk_ref,dv_ref)[kv][:,gg*128:(gg+1)*128]=jnp.concatenate([c0[0],c0[1]],axis=0).T.astype(BF)
        ret.append(ex+[merge]+both[:-1]+[lambda last=both[-1],fin=fin:(last(),fin())])
    def zero():
        acc[...]=jnp.zeros_like(acc)
    def compute(g,hooks):
        def one(it,_):
            for k in sorted(hooks):
                @pl.when(it==k)
                def _(k=k):
                    for f in hooks[k]: f()
            attend_unit(g,it,HC,info,qb,db,land[2*g],land[2*g+1],acc)
            return 0
        lax.fori_loop(0,ITERS,one,0)
        for sl in range(8):
            for kv in range(2):
                part[g][sl,kv]=(acc[info[24+sl],kv]+acc[info[32+sl],kv]+acc[info[40+sl],kv]).astype(BF)
        cp=pltpu.make_async_copy(qb.at[:,pl.ds(g*2048,2048)],dq_hbm.at[:,pl.ds(g*2048,2048)],lsem.at[4+g])
        cp.start()
        return cp
    LAG=3
    first=LAG+n
    def at(t): return [out[k][t-k*LAG] for k in range(4) if 0<=t-k*LAG<n]
    for t in range(first):
        for f in at(t): f()
        if t==4: zero()
    qc.wait(); dc.wait()
    later=[at(t) for t in range(first,3*LAG+n)]
    hooks0={OUT_IT[i]:fs for i,fs in enumerate(later)}
    cp0=compute(0,hooks0)
    zero()
    hooks1={}
    for q,its in enumerate((RET0,RET1)):
        for f,i in zip(ret[q],its): hooks1.setdefault(i,[]).append(f)
    cp1=compute(1,hooks1)
    for f in interleave(ret[2:],2): f()
    cp0.wait(); cp1.wait()
    w.drain()
    for x in exw[2:]+redw[2:]: x.drain()

OUT_IT=(2,6,10,14,18,22)
RET0=(0,4,9,9,9,12,14,16,18)
RET1=(4,10,15,15,15,18,20,22,23)

def mega(info,want,queries,keys,values,output_gradient):
    V=lambda *sh,dt=BF: pltpu.VMEM(sh,dt)
    vm=pl.BlockSpec(memory_space=pltpu.VMEM); anyspec=pl.BlockSpec(memory_space=pl.ANY)
    return pl.pallas_call(mega_kernel,
        in_specs=[pl.BlockSpec(memory_space=pltpu.SMEM),vm,vm,vm,anyspec,anyspec],
        out_specs=[anyspec,vm,vm],
        out_shape=[jax.ShapeDtypeStruct((384,4096),BF)]+[jax.ShapeDtypeStruct((512,256),BF)]*2,
        scratch_shapes=[V(16,512,128)]*4+[V(8,512,128)]*2+[V(8,512,128)]*4+[V(4,2,2,256,128),V(8,1,128,dt=jnp.int32),pltpu.SMEM((8,1,128),jnp.int32)]
            +[V(384,4096),V(384,4096),V(10,2,128,512,dt=F32)]+[V(8,2,128,512)]*2+[V(8,128,512)]*4+[V(16,128,512)]*2
            +[V(4,2,2,64,512),V(4,2,4,2,32,512),V(4,2,4,2,64,512),V(4,2,4,64,512),V(2,64,512,dt=F32),V(4,2,2,32,512),V(4,2,2,64,512)]
            +[pltpu.SemaphoreType.DMA((NSEM,)),pltpu.SemaphoreType.DMA((NSEM,)),pltpu.SemaphoreType.DMA((6,))],
        compiler_params=pltpu.CompilerParams(collective_id=0,has_side_effects=True,vmem_limit_bytes=67043328),
        name="mega")(info,want,keys,values,queries,output_gradient)
def wants(table):
    hit=(table%8).reshape(9,1)==jnp.arange(8,dtype=jnp.int32)[None]
    rows=jnp.max(jnp.where(hit,(table//8).reshape(9,1),0),axis=0)
    return jnp.pad(rows,(0,120)).reshape(1,128)
def local(queries,keys,values,output_gradient,tile_block_table):
    me=lax.axis_index("row")*8+lax.axis_index("col")
    info=make_info(tile_block_table,me)
    return mega(info,wants(tile_block_table),queries,keys,values,output_gradient)
def solution(mesh):
    from jax.sharding import PartitionSpec as P
    s=P(("row","col"),None)
    return jax.shard_map(local,mesh=mesh,in_specs=(s,)*5,out_specs=(s,)*3,check_vma=False)
```

```python
import functools
import jax, jax.numpy as jnp
from jax import lax
from jax.experimental import pallas as pl
from jax.experimental.pallas import tpu as pltpu
NT=(((1,),(1,)),((),()))
NN=(((1,),(0,)),((),()))
BF=jnp.bfloat16; F32=jnp.float32
MESH=pl.DeviceIdType.MESH
OFFS=(0,-1,1,2)

class Place:
    def __init__(self):
        self.row=lax.axis_index("row"); self.col=lax.axis_index("col")
        self.y=self.row//4; self.z=self.row%4; self.x=self.col//2; self.core=self.col%2
    def rowid(self,first,da,db):
        dy,dz=(db,da) if first=="z" else (da,db)
        return ((self.y+dy+4)%4)*4+(self.z+dz+4)%4
    def colid(self,dx,core):
        return ((self.x+dx+4)%4)*2+core
    def barrier(self):
        sem=pltpu.get_barrier_semaphore()
        for d in (1,2,3,4,5,6,7):
            pl.semaphore_signal(sem,inc=1,device_id={"col":(self.col+d)%8},device_id_type=MESH)
        for dy,dz in ((1,0),(-1,0),(0,1),(0,-1)):
            pl.semaphore_signal(sem,inc=1,device_id={"row":((self.y+dy+4)%4)*4+(self.z+dz+4)%4},device_id_type=MESH)
        pl.semaphore_wait(sem,11)

class Wires:
    def __init__(self,ssem,rsem):
        self.ssem=ssem; self.rsem=rsem; self.pending=[]
    def send(self,src,dst,si,ri,where):
        d=pltpu.make_async_remote_copy(src_ref=src,dst_ref=dst,send_sem=self.ssem.at[si],recv_sem=self.rsem.at[ri],device_id=where,device_id_type=MESH)
        d.start(); self.pending.append((src,si))
    def got(self,dst,ri,where):
        pltpu.make_async_remote_copy(src_ref=dst,dst_ref=dst,send_sem=self.ssem.at[0],recv_sem=self.rsem.at[ri],device_id=where,device_id_type=MESH).wait_recv()
    def drain(self):
        for src,si in self.pending:
            root=getattr(src,"ref",src); sh=src.shape
            ref=root.at[(0,)*(len(root.shape)-len(sh))+tuple(pl.ds(0,k) for k in sh)]
            near={"col":(lax.axis_index("col")+1)%8}
            pltpu.make_async_remote_copy(src_ref=ref,dst_ref=ref,send_sem=self.ssem.at[si],recv_sem=self.rsem.at[si],device_id=near,device_id_type=MESH).wait_send()
        self.pending=[]

AG_SEMS=20
def gather_steps(me,w,own,buf,lo,n,first,base):
    full=pl.ds(lo,n); h0=pl.ds(lo,n//2); h1=pl.ds(lo+n//2,n//2)
    def at(da,db): return {"row":me.rowid(first,da,db)}
    def spread(o,src,dst):
        w.send(src,dst,base+4+o*4,base+4+o*4,at(0,1))
        w.send(src,dst,base+5+o*4,base+5+o*4,at(0,-1))
    def piece(da,db,rows): return buf.at[me.rowid(first,da,db),rows]
    def s0():
        w.send(own,piece(0,0,full),base,base,at(1,0))
        w.send(own,piece(0,0,full),base+1,base+1,at(-1,0))
        spread(0,own,piece(0,0,full))
    def s1():
        w.got(piece(-1,0,full),base,at(-1,0))
        w.send(piece(-1,0,h0),piece(-1,0,h0),base+2,base+2,at(1,0))
        spread(1,piece(-1,0,full),piece(-1,0,full))
        w.got(piece(1,0,full),base+1,at(1,0))
        w.send(piece(1,0,h1),piece(1,0,h1),base+3,base+3,at(-1,0))
        spread(2,piece(1,0,full),piece(1,0,full))
    def turn(o):
        da=OFFS[o]; b=base+4+o*4
        w.got(piece(da,-1,full),b,at(0,-1))
        w.send(piece(da,-1,h0),piece(da,-1,h0),b+2,b+2,at(0,1))
        w.got(piece(da,1,full),b+1,at(0,1))
        w.send(piece(da,1,h1),piece(da,1,h1),b+3,b+3,at(0,-1))
    def s2(): turn(0)
    def s3():
        w.got(piece(2,0,h0),base+2,at(-1,0))
        w.got(piece(2,0,h1),base+3,at(1,0))
        spread(3,piece(2,0,full),piece(2,0,full))
    def s4(): turn(1); turn(2)
    def s5(): turn(3)
    def s6():
        for o in range(4):
            b=base+4+o*4
            w.got(piece(OFFS[o],2,h0),b+2,at(0,-1))
            w.got(piece(OFFS[o],2,h1),b+3,at(0,1))
    return [s0,s1,s2,s3,s4,s5,s6]

A2A_SEMS=13
def exchange_steps(me,w,src,relay,land,n,base):
    h0=pl.ds(0,n//2); h1=pl.ds(n//2,n//2)
    x1=me.colid(1,me.core); xm=me.colid(-1,me.core)
    def e0():
        for k in range(2):
            far=src(me.colid(2,k))
            w.send(far.at[h0],relay.at[0,k],base+k,base+k,{"col":x1})
            w.send(far.at[h1],relay.at[1,k],base+2+k,base+2+k,{"col":xm})
        for k in range(2):
            w.send(src(me.colid(1,k)),land.at[me.col],base+4+k,base+4+me.core,{"col":me.colid(1,k)})
            w.send(src(me.colid(-1,k)),land.at[me.col],base+6+k,base+6+me.core,{"col":me.colid(-1,k)})
        w.send(src(me.colid(0,1-me.core)),land.at[me.col],base+8,base+8,{"col":me.colid(0,1-me.core)})
    def e1():
        for k in range(2):
            w.got(relay.at[0,k],base+k,{"col":xm})
            w.send(relay.at[0,k],land.at[xm,h0],base+9+k,base+9+me.core,{"col":me.colid(1,k)})
            w.got(relay.at[1,k],base+2+k,{"col":x1})
            w.send(relay.at[1,k],land.at[x1,h1],base+11+k,base+11+me.core,{"col":me.colid(-1,k)})
    def e2():
        for k in range(2):
            w.got(land.at[me.colid(-1,k)],base+4+k,{"col":me.colid(-1,k)})
            w.got(land.at[me.colid(1,k)],base+6+k,{"col":me.colid(1,k)})
        w.got(land.at[me.colid(0,1-me.core)],base+8,{"col":me.colid(0,1-me.core)})
        for k in range(2):
            w.got(land.at[me.colid(2,k),h0],base+9+k,{"col":me.colid(-1,k)})
            w.got(land.at[me.colid(2,k),h1],base+11+k,{"col":me.colid(1,k)})
    return [e0,e1,e2]

RS_SEMS=20
def reduce_steps(me,w,buf,t1,t2,c,c0,t3,t4,lo,n,first,base):
    full=pl.ds(lo,n); h0=pl.ds(lo,n//2); h1=pl.ds(lo+n//2,n//2); g0=pl.ds(0,n//2); g1=pl.ds(n//2,n//2)
    def at(da,db): return {"row":me.rowid(first,da,db)}
    def piece(da,db,rows): return buf.at[me.rowid(first,da,db),rows]
    order=(3,1,2,0)
    def add(ref,other):
        ref[...]=(ref[...].astype(F32)+other[...].astype(F32)).astype(BF)
    def r0():
        for o in order:
            b=base+o*4
            w.send(piece(2,OFFS[o],h0),t1.at[o,0],b,b,at(1,0))
            w.send(piece(2,OFFS[o],h1),t1.at[o,1],b+1,b+1,at(-1,0))
    def r1():
        for o in order:
            b=base+o*4
            w.got(t1.at[o,0],b,at(-1,0)); add(piece(1,OFFS[o],h0),t1.at[o,0])
            w.got(t1.at[o,1],b+1,at(1,0)); add(piece(-1,OFFS[o],h1),t1.at[o,1])
            w.send(piece(1,OFFS[o],full),t2.at[o,0],b+2,b+2,at(1,0))
            w.send(piece(-1,OFFS[o],full),t2.at[o,1],b+3,b+3,at(-1,0))
    def r2():
        for o in order:
            b=base+o*4
            w.got(t2.at[o,0],b+2,at(-1,0)); w.got(t2.at[o,1],b+3,at(1,0))
            total=piece(0,OFFS[o],full)[...].astype(F32)+t2[o,0].astype(F32)+t2[o,1].astype(F32)
            if o==0: c0[...]=total
            else: c[o]=total.astype(BF)
            if o==3:
                w.send(c.at[3,g0],t3.at[0],base+16,base+16,at(0,1))
                w.send(c.at[3,g1],t3.at[1],base+17,base+17,at(0,-1))
    def r3():
        w.got(t3.at[0],base+16,at(0,-1)); add(c.at[2,g0],t3.at[0])
        w.got(t3.at[1],base+17,at(0,1)); add(c.at[1,g1],t3.at[1])
        w.send(c.at[2],t4.at[0],base+18,base+18,at(0,1))
        w.send(c.at[1],t4.at[1],base+19,base+19,at(0,-1))
    def r4():
        w.got(t4.at[0],base+18,at(0,-1)); w.got(t4.at[1],base+19,at(0,1))
        c0[...]+=t4[0].astype(F32)+t4[1].astype(F32)
    return [r0,r1,r2,r3,r4]

def interleave(lists,lag):
    out=[]
    span=max(k*lag+len(l) for k,l in enumerate(lists))
    for t in range(span):
        for k,l in enumerate(lists):
            s=t-k*lag
            if 0<=s<len(l): out.append(l[s])
    return out

HC=2
NCH=16//HC
ITERS=3*NCH//2
LB=4*(2*AG_SEMS+A2A_SEMS)
IB=LB+8
NSEM=IB+4*(2*RS_SEMS+A2A_SEMS)

def attend_pair(g,it,hc,info,qb,db,kb,vb,acc):
    scale=128**-0.5
    c=scale*1.4426950408889634
    rows=hc*128
    tile=it//(NCH//2)
    rsl=pl.ds(pl.multiple_of(tile*128,128),128)
    diag=info[18+tile]*128
    slots=[info[tile*3+j] for j in range(3)]
    def load(u):
        off=pl.multiple_of(g*2048+((it%(NCH//2))*2+u)*rows,rows)
        q2=qb[rsl,pl.ds(off,rows)]; d2=db[rsl,pl.ds(off,rows)]
        q=jnp.concatenate([q2[:,h*128:(h+1)*128] for h in range(hc)],axis=0)
        d=jnp.concatenate([d2[:,h*128:(h+1)*128] for h in range(hc)],axis=0)
        return off,q,d
    def products(x):
        _,q,d=x
        s=[lax.dot_general(q,kb[slots[j]],NT,preferred_element_type=F32) for j in range(3)]
        dp=[lax.dot_general(d,vb[slots[j]],NT,preferred_element_type=F32) for j in range(3)]
        return s,dp
    def soft(s,dp):
        r=lax.broadcasted_iota(jnp.int32,(rows,512),0)&127
        col=lax.broadcasted_iota(jnp.int32,(rows,512),1)
        s=[jnp.where(col<=r+diag,s[0],-jnp.inf),s[1],s[2]]
        m=jnp.max(jnp.maximum(jnp.maximum(s[0],s[1]),s[2]),axis=1,keepdims=True)*c
        p=[jnp.exp2(x*c-m) for x in s]
        l=jnp.sum(p[0]+p[1]+p[2],axis=1,keepdims=True)
        t=jnp.sum(p[0]*dp[0]+p[1]*dp[1]+p[2]*dp[2],axis=1,keepdims=True)
        inv=1.0/l
        delta=t*inv
        p=[x*inv for x in p]
        return [(p[j]*(dp[j]-delta)*scale).astype(BF) for j in range(3)],[x.astype(BF) for x in p]
    def grads(x,ds,pb):
        off,q,d=x
        dq=sum(lax.dot_general(ds[j],kb[slots[j]],NN,preferred_element_type=F32) for j in range(3)).astype(BF)
        for h in range(hc):
            qb[rsl,pl.ds(off+h*128,128)]=dq[h*128:(h+1)*128]
        qT=q.T
        dT=d.T
        for j in range(3):
            acc[tile*3+j,0]+=lax.dot_general(qT,ds[j],NN,preferred_element_type=F32)
            acc[tile*3+j,1]+=lax.dot_general(dT,pb[j],NN,preferred_element_type=F32)
    x0=load(0); w0=soft(*products(x0))
    x1=load(1); n1=products(x1)
    grads(x0,*w0)
    grads(x1,*soft(*n1))

def mega_kernel(table_ref,k_ref,v_ref,q_hbm,do_hbm,dq_hbm,dk_ref,dv_ref,*scr):
    scr=list(scr)
    take=lambda n:[scr.pop(0) for _ in range(n)]
    gat=take(4); pickd=take(2); land=take(4); relay1,wv,wsm=take(3)
    qb,db,acc=take(3); part=take(2); back=take(4); sums=take(2)
    relay2,t1,t2,c,c0,t3,t4=take(7); ssem,rsem,lsem,info,want_ref=take(5)
    me=Place(); w=Wires(ssem,rsem)
    qc=pltpu.make_async_copy(q_hbm,qb,lsem.at[2]); qc.start()
    dc=pltpu.make_async_copy(do_hbm,db,lsem.at[3]); dc.start()
    ids=[[table_ref[i,j] for j in range(3)] for i in range(3)]
    for i in range(3):
        for j in range(3): info[i*3+j]=ids[i][j]&7
        info[18+i]=((me.row*8+me.col)*3+i)%4
        for sl in range(8):
            e=jnp.int32(9)
            for j in range(3): e=jnp.where((ids[i][j]&7)==sl,i*3+j,e)
            info[24+i*8+sl]=e
    lane=lax.broadcasted_iota(jnp.int32,(1,128),1)
    mine=jnp.zeros((1,128),jnp.int32)
    for sl in range(8):
        e=jnp.int32(0)
        for i in range(3):
            for j in range(3): e=jnp.where((ids[i][j]&7)==sl,ids[i][j]//8,e)
        mine=jnp.where(lane==sl,e,mine)
    want_ref[...]=mine
    me.barrier()
    for d in range(1,8):
        w.send(want_ref,wv.at[me.col],LB+d,LB+d,{"col":(me.col+d)%8})
    def src(q,lo,n):
        return (k_ref,v_ref)[q%2].at[pl.ds(lo,n),pl.ds((q//2)*128,128)]
    def lists():
        for d in range(1,8):
            w.got(wv.at[(me.col-d+8)%8],LB+d,{"col":(me.col-d+8)%8})
        a=pltpu.make_async_copy(wv,wsm,lsem.at[0]); a.start(); a.wait()
        b=pltpu.make_async_copy(want_ref,wsm.at[me.col],lsem.at[1]); b.start(); b.wait()
    exw=[Wires(ssem,rsem) for _ in range(4)]
    out=[]
    for q in range(4):
        base=q*(2*AG_SEMS+A2A_SEMS)
        A=gather_steps(me,w,src(q,0,256),gat[q],0,256,"z",base)
        B=gather_steps(me,w,src(q,256,256),gat[q],256,256,"y",base+AG_SEMS)
        both=[(lambda a=a,b=b:(a(),b())) for a,b in zip(A,B)]
        ex=exchange_steps(me,exw[q],lambda cc,q=q:pickd[q%2].at[cc],relay1.at[q],land[q],512,base+2*AG_SEMS)
        def pick(q=q):
            if q==0: lists()
            if q>=2: exw[q-2].drain()
            gat[q][me.row]=src(q,0,512)[...]
            for cc in range(8):
                pickd[q%2][cc]=gat[q][wsm[cc,0,me.col]]
            land[q][me.col]=pickd[q%2][me.col]
        out.append(both+[pick]+ex)
    redw=[Wires(ssem,rsem) for _ in range(4)]
    ret=[]
    for q in range(4):
        base=IB+q*(2*RS_SEMS+A2A_SEMS); gg,kv=q//2,q%2
        ex=exchange_steps(me,w,lambda cc,gg=gg,kv=kv:part[gg].at[cc,kv],relay2.at[q],back[q],128,base+2*RS_SEMS)
        def merge(q=q,gg=gg,kv=kv):
            if q>=2: redw[q-2].drain()
            a=back[q]; b=sums[q%2]
            a[me.col]=part[gg][me.col,kv]
            rows=[wsm[cc,0,me.col] for cc in range(8)]
            nothing=jnp.zeros((16,256),BF)
            def block(i,_):
                r=pl.ds(pl.multiple_of((i//2)*16,16),16); ln=pl.ds(pl.multiple_of((i%2)*256,256),256)
                vals=[a[cc,r,ln] for cc in range(8)]
                for R in range(16):
                    t=[jnp.where(rows[cc]==R,vals[cc],nothing) for cc in range(8)]
                    while len(t)>1: t=[t[k]+t[k+1] for k in range(0,len(t),2)]
                    b[R,r,ln]=t[0]
                return 0
            lax.fori_loop(0,16,block,0)
        A=reduce_steps(me,redw[q],sums[q%2],t1.at[q,0],t2.at[q,0],c.at[q,0],c0.at[q,0],t3.at[q,0],t4.at[q,0],0,64,"y",base)
        B=reduce_steps(me,redw[q],sums[q%2],t1.at[q,1],t2.at[q,1],c.at[q,1],c0.at[q,1],t3.at[q,1],t4.at[q,1],64,64,"z",base+RS_SEMS)
        both=[(lambda x=x,y=y:(x(),y())) for x,y in zip(A,B)]
        def fin(q=q,gg=gg,kv=kv):
            (dk_ref,dv_ref)[kv][:,gg*128:(gg+1)*128]=jnp.concatenate([c0[q,0],c0[q,1]],axis=0).T.astype(BF)
        ret.append(ex+[merge]+both[:-1]+[lambda last=both[-1],fin=fin:(last(),fin())])
    def zero():
        acc[...]=jnp.zeros_like(acc)
    def compute(g,hooks):
        def one(it,_):
            for k in sorted(hooks):
                @pl.when(it==k)
                def _(k=k):
                    for f in hooks[k]: f()
            attend_pair(g,it,HC,info,qb,db,land[2*g],land[2*g+1],acc)
            return 0
        lax.fori_loop(0,ITERS,one,0)
        for sl in range(8):
            for kv in range(2):
                part[g][sl,kv]=(acc[info[24+sl],kv]+acc[info[32+sl],kv]+acc[info[40+sl],kv]).astype(BF)
        cp=pltpu.make_async_copy(qb.at[:,pl.ds(g*2048,2048)],dq_hbm.at[:,pl.ds(g*2048,2048)],lsem.at[4+g])
        cp.start()
        return cp
    names=("s0","s1","s2","s3","s4","s5","s6","pick","e0","e1","e2")
    go={f"{nm}{q}":out[q][i] for q in range(4) for i,nm in enumerate(names)}
    names=("x0","x1","x2","merge","r0","r1","r2","r3","r4")
    go.update({f"{nm}{q}":ret[q][i] for q in range(4) for i,nm in enumerate(names)})
    done=[]
    def run(text):
        for nm in text.split(): done.append(nm); go[nm]()
    def hooks_of(table):
        return {it:[lambda text=text: run(text)] for it,text in table}
    for text in BEFORE:
        run(text)
        if text==ZERO_AFTER: zero()
    qc.wait(); dc.wait()
    cp0=compute(0,hooks_of(UNDER0))
    zero()
    cp1=compute(1,hooks_of(UNDER1))
    for text in AFTER: run(text)
    assert len(done)==len(go) and len(set(done))==len(done)
    cp0.wait(); cp1.wait()
    w.drain()
    for x in exw[2:]+redw[2:]: x.drain()

def stagger(offsets,count,names):
    rows=[]
    for t in range(count):
        rows.append(" ".join(f"{nm}{k}" for k,o in enumerate(offsets) for i,nm in enumerate(names) if i==t-o))
    return rows
STEPS=("s0","s1","s2","s3","s4","s5","s6","pick","e0","e1","e2")
BEFORE=stagger((0,1,5,6),11,STEPS)+["e21"]
ZERO_AFTER=BEFORE[4]
UNDER0=((0,"s62 pick2 e02"),(1,"s53"),(2,"s63 pick3 e12 e03"),(5,"e13"),(11,"e22 e23"))
UNDER1=((0,"x00"),(2,"x10 x01"),(6,"x11 x20 merge0 r00"),(8,"r10"),(10,"x21 merge1 r01 r20"),(11,"r30 r11"))
AFTER=("x02","r40","r21","x12 x03","r31","x13","r41","x22 merge2 r02","r12","x23 merge3 r03","r22","r13","r32","r23","r42","r33","r43")

def mega(table,queries,keys,values,output_gradient):
    V=lambda *sh,dt=BF: pltpu.VMEM(sh,dt)
    vm=pl.BlockSpec(memory_space=pltpu.VMEM); anyspec=pl.BlockSpec(memory_space=pl.ANY)
    return pl.pallas_call(mega_kernel,
        in_specs=[pl.BlockSpec(memory_space=pltpu.SMEM),vm,vm,anyspec,anyspec],
        out_specs=[anyspec,vm,vm],
        out_shape=[jax.ShapeDtypeStruct((384,4096),BF)]+[jax.ShapeDtypeStruct((512,256),BF)]*2,
        scratch_shapes=[V(16,512,128)]*4+[V(8,512,128)]*2+[V(8,512,128)]*4+[V(4,2,2,256,128),V(8,1,128,dt=jnp.int32),pltpu.SMEM((8,1,128),jnp.int32)]
            +[V(384,4096),V(384,4096),V(10,2,128,512,dt=F32)]+[V(8,2,128,512)]*2+[V(8,128,512)]*4+[V(16,128,512)]*2
            +[V(4,2,2,64,512),V(4,2,4,2,32,512),V(4,2,4,2,64,512),V(4,2,4,64,512),V(4,2,64,512,dt=F32),V(4,2,2,32,512),V(4,2,2,64,512)]
            +[pltpu.SemaphoreType.DMA((NSEM,)),pltpu.SemaphoreType.DMA((NSEM,)),pltpu.SemaphoreType.DMA((6,)),pltpu.SMEM((48,),jnp.int32),V(1,128,dt=jnp.int32)],
        compiler_params=pltpu.CompilerParams(collective_id=0,has_side_effects=True,vmem_limit_bytes=67043328),
        name="mega")(table,keys,values,queries,output_gradient)
def local(queries,keys,values,output_gradient,tile_block_table):
    return mega(tile_block_table,queries,keys,values,output_gradient)
def solution(mesh):
    from jax.sharding import PartitionSpec as P
    s=P(("row","col"),None)
    return jax.shard_map(local,mesh=mesh,in_specs=(s,)*5,out_specs=(s,)*3,check_vma=False)
```

```python
import functools
import jax, jax.numpy as jnp
from jax import lax
from jax.experimental import pallas as pl
from jax.experimental.pallas import tpu as pltpu
NT=(((1,),(1,)),((),()))
NN=(((1,),(0,)),((),()))
BF=jnp.bfloat16; F32=jnp.float32
MESH=pl.DeviceIdType.MESH
OFFS=(0,-1,1,2)

class Place:
    def __init__(self):
        self.row=lax.axis_index("row"); self.col=lax.axis_index("col")
        self.y=self.row//4; self.z=self.row%4; self.x=self.col//2; self.core=self.col%2
    def rowid(self,first,da,db):
        dy,dz=(db,da) if first=="z" else (da,db)
        return ((self.y+dy+4)%4)*4+(self.z+dz+4)%4
    def colid(self,dx,core):
        return ((self.x+dx+4)%4)*2+core
    def barrier(self):
        sem=pltpu.get_barrier_semaphore()
        for d in (1,2,3,4,5,6,7):
            pl.semaphore_signal(sem,inc=1,device_id={"col":(self.col+d)%8},device_id_type=MESH)
        for dy,dz in ((1,0),(-1,0),(0,1),(0,-1)):
            pl.semaphore_signal(sem,inc=1,device_id={"row":((self.y+dy+4)%4)*4+(self.z+dz+4)%4},device_id_type=MESH)
        pl.semaphore_wait(sem,11)

class Wires:
    def __init__(self,ssem,rsem):
        self.ssem=ssem; self.rsem=rsem; self.pending=[]
    def send(self,src,dst,si,ri,where):
        d=pltpu.make_async_remote_copy(src_ref=src,dst_ref=dst,send_sem=self.ssem.at[si],recv_sem=self.rsem.at[ri],device_id=where,device_id_type=MESH)
        d.start(); self.pending.append((src,si))
    def got(self,dst,ri,where):
        pltpu.make_async_remote_copy(src_ref=dst,dst_ref=dst,send_sem=self.ssem.at[0],recv_sem=self.rsem.at[ri],device_id=where,device_id_type=MESH).wait_recv()
    def drain(self):
        for src,si in self.pending:
            root=getattr(src,"ref",src); sh=src.shape
            ref=root.at[(0,)*(len(root.shape)-len(sh))+tuple(pl.ds(0,k) for k in sh)]
            near={"col":(lax.axis_index("col")+1)%8}
            pltpu.make_async_remote_copy(src_ref=ref,dst_ref=ref,send_sem=self.ssem.at[si],recv_sem=self.rsem.at[si],device_id=near,device_id_type=MESH).wait_send()
        self.pending=[]

AG_SEMS=20
def gather_steps(me,w,own,buf,lo,n,first,base):
    full=pl.ds(lo,n); h0=pl.ds(lo,n//2); h1=pl.ds(lo+n//2,n//2)
    def at(da,db): return {"row":me.rowid(first,da,db)}
    def spread(o,src,dst):
        w.send(src,dst,base+4+o*4,base+4+o*4,at(0,1))
        w.send(src,dst,base+5+o*4,base+5+o*4,at(0,-1))
    def piece(da,db,rows): return buf.at[me.rowid(first,da,db),rows]
    def s0():
        w.send(own,piece(0,0,full),base,base,at(1,0))
        w.send(own,piece(0,0,full),base+1,base+1,at(-1,0))
        spread(0,own,piece(0,0,full))
    def s1():
        w.got(piece(-1,0,full),base,at(-1,0))
        w.send(piece(-1,0,h0),piece(-1,0,h0),base+2,base+2,at(1,0))
        spread(1,piece(-1,0,full),piece(-1,0,full))
        w.got(piece(1,0,full),base+1,at(1,0))
        w.send(piece(1,0,h1),piece(1,0,h1),base+3,base+3,at(-1,0))
        spread(2,piece(1,0,full),piece(1,0,full))
    def turn(o):
        da=OFFS[o]; b=base+4+o*4
        w.got(piece(da,-1,full),b,at(0,-1))
        w.send(piece(da,-1,h0),piece(da,-1,h0),b+2,b+2,at(0,1))
        w.got(piece(da,1,full),b+1,at(0,1))
        w.send(piece(da,1,h1),piece(da,1,h1),b+3,b+3,at(0,-1))
    def s2(): turn(0)
    def s3():
        w.got(piece(2,0,h0),base+2,at(-1,0))
        w.got(piece(2,0,h1),base+3,at(1,0))
        spread(3,piece(2,0,full),piece(2,0,full))
    def s4(): turn(1); turn(2)
    def s5(): turn(3)
    def s6():
        for o in range(4):
            b=base+4+o*4
            w.got(piece(OFFS[o],2,h0),b+2,at(0,-1))
            w.got(piece(OFFS[o],2,h1),b+3,at(0,1))
    return [s0,s1,s2,s3,s4,s5,s6]

A2A_SEMS=13
def exchange_steps(me,w,src,relay,land,n,base):
    h0=pl.ds(0,n//2); h1=pl.ds(n//2,n//2)
    x1=me.colid(1,me.core); xm=me.colid(-1,me.core)
    def e0():
        for k in range(2):
            far=src(me.colid(2,k))
            w.send(far.at[h0],relay.at[0,k],base+k,base+k,{"col":x1})
            w.send(far.at[h1],relay.at[1,k],base+2+k,base+2+k,{"col":xm})
        for k in range(2):
            w.send(src(me.colid(1,k)),land.at[me.col],base+4+k,base+4+me.core,{"col":me.colid(1,k)})
            w.send(src(me.colid(-1,k)),land.at[me.col],base+6+k,base+6+me.core,{"col":me.colid(-1,k)})
        w.send(src(me.colid(0,1-me.core)),land.at[me.col],base+8,base+8,{"col":me.colid(0,1-me.core)})
    def e1():
        for k in range(2):
            w.got(relay.at[0,k],base+k,{"col":xm})
            w.send(relay.at[0,k],land.at[xm,h0],base+9+k,base+9+me.core,{"col":me.colid(1,k)})
            w.got(relay.at[1,k],base+2+k,{"col":x1})
            w.send(relay.at[1,k],land.at[x1,h1],base+11+k,base+11+me.core,{"col":me.colid(-1,k)})
    def e2():
        for k in range(2):
            w.got(land.at[me.colid(-1,k)],base+4+k,{"col":me.colid(-1,k)})
            w.got(land.at[me.colid(1,k)],base+6+k,{"col":me.colid(1,k)})
        w.got(land.at[me.colid(0,1-me.core)],base+8,{"col":me.colid(0,1-me.core)})
        for k in range(2):
            w.got(land.at[me.colid(2,k),h0],base+9+k,{"col":me.colid(-1,k)})
            w.got(land.at[me.colid(2,k),h1],base+11+k,{"col":me.colid(1,k)})
    return [e0,e1,e2]

RS_SEMS=20
def reduce_steps(me,w,buf,t1,t2,c,c0,t3,t4,lo,n,first,base):
    full=pl.ds(lo,n); h0=pl.ds(lo,n//2); h1=pl.ds(lo+n//2,n//2); g0=pl.ds(0,n//2); g1=pl.ds(n//2,n//2)
    def at(da,db): return {"row":me.rowid(first,da,db)}
    def piece(da,db,rows): return buf.at[me.rowid(first,da,db),rows]
    order=(3,1,2,0)
    def add(ref,other):
        ref[...]=(ref[...].astype(F32)+other[...].astype(F32)).astype(BF)
    def r0():
        for o in order:
            b=base+o*4
            w.send(piece(2,OFFS[o],h0),t1.at[o,0],b,b,at(1,0))
            w.send(piece(2,OFFS[o],h1),t1.at[o,1],b+1,b+1,at(-1,0))
    def r1():
        for o in order:
            b=base+o*4
            w.got(t1.at[o,0],b,at(-1,0)); add(piece(1,OFFS[o],h0),t1.at[o,0])
            w.got(t1.at[o,1],b+1,at(1,0)); add(piece(-1,OFFS[o],h1),t1.at[o,1])
            w.send(piece(1,OFFS[o],full),t2.at[o,0],b+2,b+2,at(1,0))
            w.send(piece(-1,OFFS[o],full),t2.at[o,1],b+3,b+3,at(-1,0))
    def r2():
        for o in order:
            b=base+o*4
            w.got(t2.at[o,0],b+2,at(-1,0)); w.got(t2.at[o,1],b+3,at(1,0))
            total=piece(0,OFFS[o],full)[...].astype(F32)+t2[o,0].astype(F32)+t2[o,1].astype(F32)
            if o==0: c0[...]=total
            else: c[o]=total.astype(BF)
            if o==3:
                w.send(c.at[3,g0],t3.at[0],base+16,base+16,at(0,1))
                w.send(c.at[3,g1],t3.at[1],base+17,base+17,at(0,-1))
    def r3():
        w.got(t3.at[0],base+16,at(0,-1)); add(c.at[2,g0],t3.at[0])
        w.got(t3.at[1],base+17,at(0,1)); add(c.at[1,g1],t3.at[1])
        w.send(c.at[2],t4.at[0],base+18,base+18,at(0,1))
        w.send(c.at[1],t4.at[1],base+19,base+19,at(0,-1))
    def r4():
        w.got(t4.at[0],base+18,at(0,-1)); w.got(t4.at[1],base+19,at(0,1))
        c0[...]+=t4[0].astype(F32)+t4[1].astype(F32)
    return [r0,r1,r2,r3,r4]

def interleave(lists,lag):
    out=[]
    span=max(k*lag+len(l) for k,l in enumerate(lists))
    for t in range(span):
        for k,l in enumerate(lists):
            s=t-k*lag
            if 0<=s<len(l): out.append(l[s])
    return out

HC=2
NCH=16//HC
ITERS=3*NCH//2
LB=4*(2*AG_SEMS+A2A_SEMS)
IB=LB+8
NSEM=IB+4*(2*RS_SEMS+A2A_SEMS)

def attend_pair(g,it,hc,info,qb,db,kb,vb,acc):
    scale=128**-0.5
    c=scale*1.4426950408889634
    rows=hc*128
    tile=it//(NCH//2)
    rsl=pl.ds(pl.multiple_of(tile*128,128),128)
    diag=info[18+tile]*128
    slots=[info[tile*3+j] for j in range(3)]
    def load(u):
        off=pl.multiple_of(g*2048+((it%(NCH//2))*2+u)*rows,rows)
        q2=qb[rsl,pl.ds(off,rows)]; d2=db[rsl,pl.ds(off,rows)]
        q=jnp.concatenate([q2[:,h*128:(h+1)*128] for h in range(hc)],axis=0)
        d=jnp.concatenate([d2[:,h*128:(h+1)*128] for h in range(hc)],axis=0)
        return off,q,d
    def products(x):
        _,q,d=x
        s=[lax.dot_general(q,kb[slots[j]],NT,preferred_element_type=F32) for j in range(3)]
        dp=[lax.dot_general(d,vb[slots[j]],NT,preferred_element_type=F32) for j in range(3)]
        return s,dp
    def soft(s,dp):
        r=lax.broadcasted_iota(jnp.int32,(rows,512),0)&127
        col=lax.broadcasted_iota(jnp.int32,(rows,512),1)
        s=[jnp.where(col<=r+diag,s[0],-jnp.inf),s[1],s[2]]
        m=jnp.max(jnp.maximum(jnp.maximum(s[0],s[1]),s[2]),axis=1,keepdims=True)*c
        p=[jnp.exp2(x*c-m) for x in s]
        l=jnp.sum(p[0]+p[1]+p[2],axis=1,keepdims=True)
        t=jnp.sum(p[0]*dp[0]+p[1]*dp[1]+p[2]*dp[2],axis=1,keepdims=True)
        inv=1.0/l
        delta=t*inv
        p=[x*inv for x in p]
        return [(p[j]*(dp[j]-delta)*scale).astype(BF) for j in range(3)],[x.astype(BF) for x in p]
    def grads(x,ds,pb):
        off,q,d=x
        dq=sum(lax.dot_general(ds[j],kb[slots[j]],NN,preferred_element_type=F32) for j in range(3)).astype(BF)
        for h in range(hc):
            qb[rsl,pl.ds(off+h*128,128)]=dq[h*128:(h+1)*128]
        qT=q.T
        dT=d.T
        for j in range(3):
            acc[tile*3+j,0]+=lax.dot_general(qT,ds[j],NN,preferred_element_type=F32)
            acc[tile*3+j,1]+=lax.dot_general(dT,pb[j],NN,preferred_element_type=F32)
    x0=load(0); w0=soft(*products(x0))
    x1=load(1); n1=products(x1)
    grads(x0,*w0)
    grads(x1,*soft(*n1))

def mega_kernel(table_ref,k_ref,v_ref,q_hbm,do_hbm,dq_hbm,dk_ref,dv_ref,*scr):
    scr=list(scr)
    take=lambda n:[scr.pop(0) for _ in range(n)]
    gat=take(4); pickd=take(2); land=take(4); relay1,wv,wsm=take(3)
    qb,db,acc=take(3); part=take(2); back=take(4); sums=take(2)
    relay2,t1,t2,c,c0,t3,t4=take(7); ssem,rsem,lsem,info,want_ref=take(5)
    me=Place(); w=Wires(ssem,rsem)
    qc=pltpu.make_async_copy(q_hbm,qb,lsem.at[2]); qc.start()
    dc=pltpu.make_async_copy(do_hbm,db,lsem.at[3]); dc.start()
    ids=[[table_ref[i,j] for j in range(3)] for i in range(3)]
    for i in range(3):
        for j in range(3): info[i*3+j]=ids[i][j]&7
        info[18+i]=((me.row*8+me.col)*3+i)%4
        for sl in range(8):
            e=jnp.int32(9)
            for j in range(3): e=jnp.where((ids[i][j]&7)==sl,i*3+j,e)
            info[24+i*8+sl]=e
    lane=lax.broadcasted_iota(jnp.int32,(1,128),1)
    mine=jnp.zeros((1,128),jnp.int32)
    for sl in range(8):
        e=jnp.int32(0)
        for i in range(3):
            for j in range(3): e=jnp.where((ids[i][j]&7)==sl,ids[i][j]//8,e)
        mine=jnp.where(lane==sl,e,mine)
    want_ref[...]=mine
    me.barrier()
    for d in range(1,8):
        w.send(want_ref,wv.at[me.col],LB+d,LB+d,{"col":(me.col+d)%8})
    def src(q,lo,n):
        return (k_ref,v_ref)[q%2].at[pl.ds(lo,n),pl.ds((q//2)*128,128)]
    def lists():
        for d in range(1,8):
            w.got(wv.at[(me.col-d+8)%8],LB+d,{"col":(me.col-d+8)%8})
        a=pltpu.make_async_copy(wv,wsm,lsem.at[0]); a.start(); a.wait()
        b=pltpu.make_async_copy(want_ref,wsm.at[me.col],lsem.at[1]); b.start(); b.wait()
    exw=[Wires(ssem,rsem) for _ in range(4)]
    out=[]
    for q in range(4):
        base=q*(2*AG_SEMS+A2A_SEMS)
        A=gather_steps(me,w,src(q,0,256),gat[q],0,256,"z",base)
        B=gather_steps(me,w,src(q,256,256),gat[q],256,256,"y",base+AG_SEMS)
        both=[(lambda a=a,b=b:(a(),b())) for a,b in zip(A,B)]
        ex=exchange_steps(me,exw[q],lambda cc,q=q:pickd[q%2].at[cc],relay1.at[q],land[q],512,base+2*AG_SEMS)
        def pick(q=q):
            if q==0: lists()
            if q>=2: exw[q-2].drain()
            gat[q][me.row]=src(q,0,512)[...]
            for cc in range(8):
                pickd[q%2][cc]=gat[q][wsm[cc,0,me.col]]
            land[q][me.col]=pickd[q%2][me.col]
        out.append(both+[pick]+ex)
    redw=[Wires(ssem,rsem) for _ in range(4)]
    ret=[]
    for q in range(4):
        base=IB+q*(2*RS_SEMS+A2A_SEMS); gg,kv=q//2,q%2
        ex=exchange_steps(me,w,lambda cc,gg=gg,kv=kv:part[gg].at[cc,kv],relay2.at[q],back[q],128,base+2*RS_SEMS)
        def merge(q=q,gg=gg,kv=kv):
            if q>=2: redw[q-2].drain()
            a=back[q]; b=sums[q%2]
            a[me.col]=part[gg][me.col,kv]
            rows=[wsm[cc,0,me.col] for cc in range(8)]
            nothing=jnp.zeros((16,256),BF)
            def block(i,_):
                r=pl.ds(pl.multiple_of((i//2)*16,16),16); ln=pl.ds(pl.multiple_of((i%2)*256,256),256)
                vals=[a[cc,r,ln] for cc in range(8)]
                for R in range(16):
                    t=[jnp.where(rows[cc]==R,vals[cc],nothing) for cc in range(8)]
                    while len(t)>1: t=[t[k]+t[k+1] for k in range(0,len(t),2)]
                    b[R,r,ln]=t[0]
                return 0
            lax.fori_loop(0,16,block,0)
        A=reduce_steps(me,redw[q],sums[q%2],t1.at[q,0],t2.at[q,0],c.at[q,0],c0.at[q,0],t3.at[q,0],t4.at[q,0],0,64,"y",base)
        B=reduce_steps(me,redw[q],sums[q%2],t1.at[q,1],t2.at[q,1],c.at[q,1],c0.at[q,1],t3.at[q,1],t4.at[q,1],64,64,"z",base+RS_SEMS)
        both=[(lambda x=x,y=y:(x(),y())) for x,y in zip(A,B)]
        def fin(q=q,gg=gg,kv=kv):
            (dk_ref,dv_ref)[kv][:,gg*128:(gg+1)*128]=jnp.concatenate([c0[q,0],c0[q,1]],axis=0).T.astype(BF)
        ret.append(ex+[merge]+both[:-1]+[lambda last=both[-1],fin=fin:(last(),fin())])
    def zero():
        acc[...]=jnp.zeros_like(acc)
    def compute(g,hooks):
        def one(it,_):
            for k in sorted(hooks):
                @pl.when(it==k)
                def _(k=k):
                    for f in hooks[k]: f()
            attend_pair(g,it,HC,info,qb,db,land[2*g],land[2*g+1],acc)
            return 0
        lax.fori_loop(0,ITERS,one,0)
        for sl in range(8):
            for kv in range(2):
                part[g][sl,kv]=(acc[info[24+sl],kv]+acc[info[32+sl],kv]+acc[info[40+sl],kv]).astype(BF)
        cp=pltpu.make_async_copy(qb.at[:,pl.ds(g*2048,2048)],dq_hbm.at[:,pl.ds(g*2048,2048)],lsem.at[4+g])
        cp.start()
        return cp
    names=("s0","s1","s2","s3","s4","s5","s6","pick","e0","e1","e2")
    go={f"{nm}{q}":out[q][i] for q in range(4) for i,nm in enumerate(names)}
    names=("x0","x1","x2","merge","r0","r1","r2","r3","r4")
    go.update({f"{nm}{q}":ret[q][i] for q in range(4) for i,nm in enumerate(names)})
    done=[]
    def run(text):
        for nm in text.split(): done.append(nm); go[nm]()
    def hooks_of(table):
        return {it:[lambda text=text: run(text)] for it,text in table}
    for text in BEFORE:
        run(text)
        if text==ZERO_AFTER: zero()
    qc.wait(); dc.wait()
    cp0=compute(0,hooks_of(UNDER0))
    zero()
    cp1=compute(1,hooks_of(UNDER1))
    for text in AFTER: run(text)
    assert len(done)==len(go) and len(set(done))==len(done)
    cp0.wait(); cp1.wait()
    w.drain()
    for x in exw[2:]+redw[2:]: x.drain()

def stagger(offsets,count,names):
    rows=[]
    for t in range(count):
        rows.append(" ".join(f"{nm}{k}" for k,o in enumerate(offsets) for i,nm in enumerate(names) if i==t-o))
    return rows
STEPS=("s0","s1","s2","s3","s4","s5","s6","pick","e0","e1","e2")
BEFORE=stagger((0,1,8,9),11,STEPS)+["e21"]
ZERO_AFTER=BEFORE[4]
UNDER0=((0,"s32 s23"),(1,"s42 s33"),(2,"s52 s43"),(3,"s62 s53 pick2 e02"),(5,"s63 pick3 e12 e03"),(7,"e13"),(11,"e22 e23"))
UNDER1=((0,"x00"),(2,"x10 x01"),(6,"x11 x20 merge0 r00"),(8,"r10"),(10,"x21 merge1 r01 r20"),(11,"r30 r11"))
AFTER=("x02","r40","r21","x12 x03","r31","x13","r41","x22 merge2 r02","r12","x23 merge3 r03","r22","r13","r32","r23","r42","r33","r43")

def mega(table,queries,keys,values,output_gradient):
    V=lambda *sh,dt=BF: pltpu.VMEM(sh,dt)
    vm=pl.BlockSpec(memory_space=pltpu.VMEM); anyspec=pl.BlockSpec(memory_space=pl.ANY)
    return pl.pallas_call(mega_kernel,
        in_specs=[pl.BlockSpec(memory_space=pltpu.SMEM),vm,vm,anyspec,anyspec],
        out_specs=[anyspec,vm,vm],
        out_shape=[jax.ShapeDtypeStruct((384,4096),BF)]+[jax.ShapeDtypeStruct((512,256),BF)]*2,
        scratch_shapes=[V(16,512,128)]*4+[V(8,512,128)]*2+[V(8,512,128)]*4+[V(4,2,2,256,128),V(8,1,128,dt=jnp.int32),pltpu.SMEM((8,1,128),jnp.int32)]
            +[V(384,4096),V(384,4096),V(10,2,128,512,dt=F32)]+[V(8,2,128,512)]*2+[V(8,128,512)]*4+[V(16,128,512)]*2
            +[V(4,2,2,64,512),V(4,2,4,2,32,512),V(4,2,4,2,64,512),V(4,2,4,64,512),V(4,2,64,512,dt=F32),V(4,2,2,32,512),V(4,2,2,64,512)]
            +[pltpu.SemaphoreType.DMA((NSEM,)),pltpu.SemaphoreType.DMA((NSEM,)),pltpu.SemaphoreType.DMA((6,)),pltpu.SMEM((48,),jnp.int32),V(1,128,dt=jnp.int32)],
        compiler_params=pltpu.CompilerParams(collective_id=0,has_side_effects=True,vmem_limit_bytes=67043328),
        name="mega")(table,keys,values,queries,output_gradient)
def local(queries,keys,values,output_gradient,tile_block_table):
    return mega(tile_block_table,queries,keys,values,output_gradient)
def solution(mesh):
    from jax.sharding import PartitionSpec as P
    s=P(("row","col"),None)
    return jax.shard_map(local,mesh=mesh,in_specs=(s,)*5,out_specs=(s,)*3,check_vma=False)
```
